256 devices in a mesh: row: 8 (over x, core), col: 32 (over y, z).
Axes of the slice: x: 4, y: 4, z: 8, core: 2. Of those that a mesh axis runs over, the one named last changes fastest.
Arguments:
- right_sides: bfloat16 [8192, 64, 128], P(('row', 'col')), may hold values from -7 to 7
- weights_fine: bfloat16 [8192, 3, 128, 128], P(('row', 'col')), may hold values from 0 to 2
- columns_fine: int32 [8192, 3], P(('row', 'col')), may hold values from 0 to 8191, as said below
- degree_fine: float32 [8192, 128], P(('row', 'col')), may hold values from 0.05 to 0.5
- owners_fine: int32 [8192, 128], P(('row', 'col')), may hold values from 0 to 255, as said below
- slots_fine: int32 [8192, 128], P(('row', 'col')), may hold values from 0 to 1023
- weights_second: bfloat16 [2048, 3, 128, 128], P(('row', 'col')), may hold values from 0 to 8
- columns_second: int32 [2048, 3], P(('row', 'col')), may hold values from 0 to 2047, as said below
- degree_second: float32 [2048, 128], P(('row', 'col')), may hold values from 0.2 to 2
- owners_second: int32 [2048, 128], P(('row', 'col')), may hold values from 0 to 255, as said below
- slots_second: int32 [2048, 128], P(('row', 'col')), may hold values from 0 to 255
- weights_third: bfloat16 [512, 3, 128, 128], P(('row', 'col')), may hold values from 0 to 32
- columns_third: int32 [512, 3], P(('row', 'col')), may hold values from 0 to 511, as said below
- degree_third: float32 [512, 128], P(('row', 'col')), may hold values from 0.8 to 8
- owners_third: int32 [512, 128], P(('row', 'col')), may hold values from 0 to 255, as said below
- slots_third: int32 [512, 128], P(('row', 'col')), may hold values from 0 to 127
- coarse_inverse: bfloat16 [32768, 4096], P(('row', 'col')), may hold values from -1 to 1, as said below
Outputs:
- solution: float32 [8192, 64, 128], P(('row', 'col'))
The draws below stay inside these ranges and needn't reach their ends.
Inputs may be any that keep to these rules, and one draw needn't show every extreme that they name: `columns_fine`: every entry lies within 2 blocks of its own row block's index, on the same level. `columns_second`: every entry lies within 2 blocks of its own row block's index, on the same level. `columns_third`: every entry lies within 2 blocks of its own row block's index, on the same level. `owners_fine`: each entry is the device holding the vertex or the one just before or after it in device order. `owners_second`: each entry is the device holding the vertex or the one just before or after it in device order. `owners_third`: each entry is the device holding the vertex or the one just before or after it in device order. `coarse_inverse`: each row group's block is symmetric.
All inputs are finite; a program needn't handle non-finite values.
Results may differ from the reference program's by a relative error of at most 0.0003.
Values may be sent and summed in bfloat16 or wider, within the bound.
No kernel may reach another device: no remote copies, remote signals or barrier semaphores. Data moves between devices by JAX's collectives and lax.ppermute only.
A program may use at most 64 MiB of HBM per device.

```python
import math
import jax
import jax.numpy as jnp
from jax import lax

RHS_COUNT = 64
BS = 128
K = 3
HB = 2
SWEEPS = 2
NB2 = 2
NB1 = 8
NB0 = 32
C3 = 128
M3 = 4096
N_ROW = 8
DEVICES = 256


def arrange_columns(drawn, blocks_here):
    total = blocks_here * DEVICES
    spread = 2 * HB + 1
    scores = drawn * spread + jnp.arange(spread, dtype=jnp.int32)[None, :]
    chosen = jnp.argsort(scores, axis=1)[:, :K].astype(jnp.int32) - HB
    rows_here = jnp.arange(total, dtype=jnp.int32)[:, None]
    target = rows_here + chosen
    outside = (target < 0) | (target >= total)
    return jnp.where(outside, rows_here - chosen, target).astype(jnp.int32)


def arrange_owners(drawn, blocks_here):
    total = blocks_here * DEVICES
    device = (jnp.arange(total, dtype=jnp.int32) // blocks_here)[:, None]
    moved = jnp.where(drawn == 6, -1, jnp.where(drawn == 7, 1, 0))
    return jnp.clip(device + moved, 0, DEVICES - 1).astype(jnp.int32)


def draw_right_sides(key, part):
    total_blocks = NB0 * DEVICES
    vertex = (jnp.arange(total_blocks, dtype=jnp.float32)[:, None, None] * BS + jnp.arange(BS, dtype=jnp.float32)[None, None, :]) / (total_blocks * BS * 1.0)
    frequency = jax.random.randint(jax.random.fold_in(key, 41), (RHS_COUNT,), 1, 4).astype(jnp.float32)
    phase = jax.random.uniform(jax.random.fold_in(key, 42), (RHS_COUNT,), jnp.float32, -3.14159, 3.14159)
    amplitude = jax.random.uniform(jax.random.fold_in(key, 43), (RHS_COUNT,), jnp.float32, 0.25, 0.5)
    wave = jnp.sin(6.283185 * frequency[None, :, None] * vertex + phase[None, :, None])
    shape = (total_blocks, RHS_COUNT, BS)
    flips = jax.random.randint(jax.random.fold_in(key, 45), (RHS_COUNT,), 0, 2)
    signs = jnp.where(flips == 0, -1.0, 1.0).astype(jnp.float32)
    smooth = (signs * amplitude)[None, :, None] * wave
    rough = jnp.clip(jax.random.normal(jax.random.fold_in(key, 44), shape, jnp.float32), -6.0, 6.0)
    return (smooth + rough).astype(jnp.bfloat16)


def draw_columns_fine(key, part):
    drawn = jax.random.randint(jax.random.fold_in(key, 11), (NB0 * DEVICES, 2 * HB + 1), 0, 1 << 20)
    return arrange_columns(drawn, NB0)


def draw_columns_second(key, part):
    drawn = jax.random.randint(jax.random.fold_in(key, 12), (NB1 * DEVICES, 2 * HB + 1), 0, 1 << 20)
    return arrange_columns(drawn, NB1)


def draw_columns_third(key, part):
    drawn = jax.random.randint(jax.random.fold_in(key, 13), (NB2 * DEVICES, 2 * HB + 1), 0, 1 << 20)
    return arrange_columns(drawn, NB2)


def draw_owners_fine(key, part):
    drawn = jax.random.randint(jax.random.fold_in(key, 21), (NB0 * DEVICES, BS), 0, 8)
    return arrange_owners(drawn, NB0)


def draw_owners_second(key, part):
    drawn = jax.random.randint(jax.random.fold_in(key, 22), (NB1 * DEVICES, BS), 0, 8)
    return arrange_owners(drawn, NB1)


def draw_owners_third(key, part):
    drawn = jax.random.randint(jax.random.fold_in(key, 23), (NB2 * DEVICES, BS), 0, 8)
    return arrange_owners(drawn, NB2)


def draw_coarse_inverse(key, part):
    groups = DEVICES * C3 // M3
    inner = jax.random.fold_in(key, 31)
    raw = jnp.clip(jax.random.normal(inner, (groups, M3, M3), jnp.float32), -3.0, 3.0)
    symmetric = 0.5 * (raw + jnp.transpose(raw, (0, 2, 1))) * (0.025 / jnp.sqrt(M3 * 1.0))
    matrix = symmetric + 0.05 * jnp.eye(M3, dtype=jnp.float32)[None, :, :]
    return matrix.reshape(groups * M3, M3).astype(jnp.bfloat16)


def place_ends(values, rng, smallest, top_value):
    extent = values.shape
    index_at = [jax.random.randint(jax.random.fold_in(rng, axis), (), 0, extent[axis]) for axis in range(len(extent))]
    values = values.at[tuple(index_at)].set(smallest)
    longest = extent.index(max(extent))
    index_at[longest] = (index_at[longest] + 1) % extent[longest]
    return values.at[tuple(index_at)].set(top_value)


def block_levels(key, extent, pieces, least, largest):
    loudness = 1.0
    for dim, parts in pieces:
        draws = jax.random.uniform(jax.random.fold_in(jax.random.fold_in(key, 6), dim), (parts,), jnp.float32, least / len(pieces), largest / len(pieces))
        loudness = loudness * jnp.repeat(jnp.exp(draws), extent[dim] // parts).reshape((-1,) + (1,) * (len(extent) - 1 - dim))
    return loudness


def setup_inputs(seed: int = 0) -> dict:
    keys = jax.random.split(jax.random.key(seed), 18)
    right_sides = draw_right_sides(jax.random.fold_in(keys[17], 71), 0)
    weights_fine = jnp.clip(2.0 * jax.random.uniform(keys[1], (NB0 * DEVICES, K, BS, BS), jnp.float32) ** block_levels(keys[1], (NB0 * DEVICES, K, BS, BS), ((0, 256),), -0.2, 0.2), 0.0, 2.0).astype(jnp.bfloat16)
    columns_fine = draw_columns_fine(jax.random.fold_in(keys[17], 71), 0)
    degree_fine = jnp.clip(jnp.exp(math.log(0.5) - 2.3025851 * jax.random.uniform(keys[3], (NB0 * DEVICES, BS), jnp.float32) ** block_levels(keys[3], (NB0 * DEVICES, BS), ((0, 256),), -0.2, 0.2)), 0.05, 0.5)
    owners_fine = draw_owners_fine(jax.random.fold_in(keys[17], 71), 0)
    slots_fine = place_ends(jax.random.randint(keys[5], (NB0 * DEVICES, BS), 0, NB1 * BS), jax.random.fold_in(keys[5], 1), 0, (NB1 * BS) - 1).astype(jnp.int32)
    weights_second = jnp.clip(8.0 * jax.random.uniform(keys[6], (NB1 * DEVICES, K, BS, BS), jnp.float32) ** block_levels(keys[6], (NB1 * DEVICES, K, BS, BS), ((0, 256),), -0.2, 0.2), 0.0, 8.0).astype(jnp.bfloat16)
    columns_second = draw_columns_second(jax.random.fold_in(keys[17], 71), 0)
    degree_second = jnp.clip(jnp.exp(math.log(2.0) - 2.3025851 * jax.random.uniform(keys[8], (NB1 * DEVICES, BS), jnp.float32) ** block_levels(keys[8], (NB1 * DEVICES, BS), ((0, 256),), -0.2, 0.2)), 0.2, 2.0)
    owners_second = draw_owners_second(jax.random.fold_in(keys[17], 71), 0)
    slots_second = place_ends(jax.random.randint(keys[10], (NB1 * DEVICES, BS), 0, NB2 * BS), jax.random.fold_in(keys[10], 1), 0, (NB2 * BS) - 1).astype(jnp.int32)
    weights_third = jnp.clip(32.0 * jax.random.uniform(keys[11], (NB2 * DEVICES, K, BS, BS), jnp.float32) ** block_levels(keys[11], (NB2 * DEVICES, K, BS, BS), ((0, 256),), -0.2, 0.2), 0.0, 32.0).astype(jnp.bfloat16)
    columns_third = draw_columns_third(jax.random.fold_in(keys[17], 71), 0)
    degree_third = jnp.clip(jnp.exp(math.log(8.0) - 2.3025851 * jax.random.uniform(keys[13], (NB2 * DEVICES, BS), jnp.float32) ** block_levels(keys[13], (NB2 * DEVICES, BS), ((0, 256),), -0.2, 0.2)), 0.8, 8.0)
    owners_third = draw_owners_third(jax.random.fold_in(keys[17], 71), 0)
    slots_third = place_ends(jax.random.randint(keys[15], (NB2 * DEVICES, BS), 0, C3), jax.random.fold_in(keys[15], 1), 0, C3 - 1).astype(jnp.int32)
    coarse_inverse = draw_coarse_inverse(jax.random.fold_in(keys[17], 71), 0)
    return dict(right_sides=right_sides, weights_fine=weights_fine, columns_fine=columns_fine, degree_fine=degree_fine, owners_fine=owners_fine, slots_fine=slots_fine, weights_second=weights_second, columns_second=columns_second, degree_second=degree_second, owners_second=owners_second, slots_second=slots_second, weights_third=weights_third, columns_third=columns_third, degree_third=degree_third, owners_third=owners_third, slots_third=slots_third, coarse_inverse=coarse_inverse)


damping = 0.8


def gather_rows(blocks):
    return jnp.transpose(blocks, (0, 2, 1)).reshape(-1, RHS_COUNT)


def make_blocks(rows_data):
    return jnp.transpose(rows_data.reshape(-1, BS, RHS_COUNT), (0, 2, 1))


def complete_diagonal_entries(weights, shift):
    return shift + jnp.sum(weights, axis=(1, 2), dtype=jnp.float32) / (K * BS)


def apply_operator(current_iterate, weights, columns, degree):
    total = current_iterate.shape[0]
    per_device = total // DEVICES
    rounded = lax.optimization_barrier(current_iterate.astype(jnp.bfloat16))
    widened = rounded.astype(jnp.float32)
    shaped_weights = weights.reshape(DEVICES, per_device, K, BS, BS)
    shaped_columns = columns.reshape(DEVICES, per_device, K)

    def per_block(packed):
        block_weights, block_columns = packed
        picked = widened[block_columns]
        return jnp.einsum("nkrb,nkbc->nrc", picked, block_weights.astype(jnp.float32), precision=lax.Precision.HIGHEST)

    product = lax.map(per_block, (shaped_weights, shaped_columns)).reshape(total, RHS_COUNT, BS)
    return degree[:, None, :] * current_iterate - product / (K * BS)


def reference(right_sides, weights_fine, columns_fine, degree_fine, owners_fine, slots_fine, weights_second, columns_second, degree_second, owners_second, slots_second, weights_third, columns_third, degree_third, owners_third, slots_third, coarse_inverse):
    levels = [(weights_fine, columns_fine, complete_diagonal_entries(weights_fine, degree_fine), owners_fine, slots_fine, NB1 * BS),
              (weights_second, columns_second, complete_diagonal_entries(weights_second, degree_second), owners_second, slots_second, NB2 * BS),
              (weights_third, columns_third, complete_diagonal_entries(weights_third, degree_third), owners_third, slots_third, C3)]
    source = right_sides.astype(jnp.float32)
    stored = []
    coarse_rows = None
    for position in range(3):
        weights, columns, degree, aggregate_owners, slots, coarse_count = levels[position]
        scale = degree[:, None, :]
        current_iterate = damping * source / scale
        for repeat in range(SWEEPS - 1):
            current_iterate = current_iterate + damping * (source - apply_operator(current_iterate, weights, columns, degree)) / scale
        residual = source - apply_operator(current_iterate, weights, columns, degree)
        stored.append((current_iterate, source))
        targets = (aggregate_owners * coarse_count + slots).reshape(-1).astype(jnp.int32)
        coarse_rows = jax.ops.segment_sum(gather_rows(residual), targets, num_segments=DEVICES * coarse_count)
        if position < 2:
            source = make_blocks(coarse_rows)
    aggregated_values = lax.optimization_barrier(coarse_rows.astype(jnp.bfloat16)).astype(jnp.float32).reshape(N_ROW, M3, RHS_COUNT)
    inverse_matrix = coarse_inverse.astype(jnp.float32).reshape(N_ROW, M3, M3)
    coarse_correction_rows = jnp.einsum("dut,dtx->dux", inverse_matrix, aggregated_values, precision=lax.Precision.HIGHEST).reshape(-1, RHS_COUNT)
    current_iterate = None
    for position in (2, 1, 0):
        weights, columns, degree, aggregate_owners, slots, coarse_count = levels[position]
        current_iterate, source = stored[position]
        targets = (aggregate_owners * coarse_count + slots).reshape(-1).astype(jnp.int32)
        current_iterate = current_iterate + make_blocks(coarse_correction_rows[targets])
        scale = degree[:, None, :]
        for repeat in range(SWEEPS):
            current_iterate = current_iterate + damping * (source - apply_operator(current_iterate, weights, columns, degree)) / scale
        coarse_correction_rows = gather_rows(current_iterate)
    return current_iterate
```

```python
import functools

import jax
import jax.numpy as jnp
from jax import lax
from jax.experimental import pallas as pl
from jax.experimental.pallas import tpu as pltpu
from jax.sharding import PartitionSpec as P

BS = 128
R = 64
K = 3
HB = 2
NB2 = 2
NB1 = 8
NB0 = 32
C3 = 128
AXES = ("row", "col")
EDGE = 2 * HB
damping = 0.8
bf16 = jnp.bfloat16
f32 = jnp.float32


def passed_along(value, steps):
    count = lax.axis_size(AXES)
    initial, last = (max(0, -steps), min(count, count - steps))
    return lax.ppermute(value, AXES, [(s, s + steps) for s in range(initial, last)])


def both_ways(up, down):
    return passed_along(up, 1), passed_along(down, -1)


def split(x):
    high = x.astype(bf16)
    return high, (x - high.astype(f32)).astype(bf16)


def full_diagonal(weights, shift):
    return shift + jnp.sum(weights, axis=(1, 2), dtype=f32) / (K * BS)


def edge_rows(weights, diagonal, near, first):
    n = weights.shape[0]
    w = weights[:HB] if first else weights[n - HB :]
    g = diagonal[:EDGE] if first else diagonal[n - EDGE :]
    c = near[:HB] if first else near[n - HB :]
    c = jnp.pad(c.reshape(1, HB * K).astype(bf16), ((0, 7), (0, BS - HB * K)))
    return [w.reshape(HB * K * BS, BS), *split(g), c]


G_AT = HB * K * BS
C_AT = G_AT + 2 * EDGE
STATIC = C_AT + 8


def near_of(static_rows, offset):
    return static_rows[offset + C_AT, : HB * K].astype(jnp.int32).reshape(HB, K)


def blocks_product(v_ref, w, near_ref, row, base):
    parts = [v_ref[base + near_ref[row * K + k]] for k in range(K)]
    return jnp.dot(jnp.concatenate(parts, axis=1), w, preferred_element_type=f32) * (1.0 / (K * BS))


def halo_diag(ref, offset, i):
    at = offset + G_AT
    return ref[at + i : at + i + 1, :].astype(f32) + ref[at + EDGE + i : at + EDGE + i + 1, :].astype(f32)


def halo_weights(ref, offset, i):
    return ref[offset + i * K * BS : offset + (i + 1) * K * BS, :]


def load_weights(w_hbm, w_ref, sem, n, chunks):
    size = n // chunks
    return [
        pltpu.make_async_copy(w_hbm.at[pl.ds(c * size, size)], w_ref.at[pl.ds(c * size, size)], sem.at[c])
        for c in range(chunks)
    ]


def down_kernel(
    n, nc, so, chunks,
    near_ref, f_ref, g_ref, t_ref, flo_ref, fhi_ref, slo_ref, shi_ref, w_hbm,
    x_ref, down_ref, mid_ref, up_ref,
    w_ref, v0_ref, v1_ref, r_ref, acc_ref, sem,
):
    copies = load_weights(w_hbm, w_ref, sem, n, chunks)
    for c in copies:
        c.start()
    size = n // chunks

    def start_of(b):
        return f_ref[b].astype(f32) * (damping / g_ref[pl.ds(b, 1), :])

    def fill(b, carry):
        v0_ref[b + EDGE] = start_of(b).astype(bf16)
        return carry

    lax.fori_loop(0, n, fill, 0, unroll=2)
    edges = {}
    for side, fr, sr in ((0, flo_ref, slo_ref), (1, fhi_ref, shi_ref)):
        for i in range(EDGE):
            g = halo_diag(sr, so, i)
            s = jnp.where(g > 0, damping / g, 0.0)
            x0 = fr[i * R : (i + 1) * R, :].astype(f32) * s
            v0_ref[i + side * (n + EDGE)] = x0.astype(bf16)
            edges[side, i] = (s, x0)
    for side, sr in ((0, slo_ref), (1, shi_ref)):
        for i in range(HB):
            s, x0 = edges[side, i + HB * (1 - side)]
            j = i + side * (n + HB)
            p = blocks_product(v0_ref, halo_weights(sr, so, i), near_ref, j, j)
            v1_ref[j] = (1.2 * x0 + s * p).astype(bf16)

    def first(b, carry):
        p = blocks_product(v0_ref, w_ref[b], near_ref, b + HB, b + HB)
        s = damping / g_ref[pl.ds(b, 1), :]
        x = 1.2 * (f_ref[b].astype(f32) * s) + s * p
        x_ref[b] = x
        v1_ref[b + HB] = x.astype(bf16)
        return carry

    for c in range(chunks):
        copies[c].wait()
        lax.fori_loop(c * size, (c + 1) * size, first, 0, unroll=4 if size % 4 == 0 else 2)

    def residual(b, half):
        p = blocks_product(v1_ref, w_ref[b], near_ref, b + HB, b)
        return f_ref[b].astype(f32) - g_ref[pl.ds(b, 1), :] * x_ref[b] + p

    def second(q, carry):
        r_ref[q] = jnp.concatenate([residual(2 * q, 0), residual(2 * q + 1, 1)], axis=1).astype(bf16)
        return carry

    lax.fori_loop(0, n // 2, second, 0, unroll=2)

    highs = 3 * nc // 2
    group = 4
    acc_ref[...] = jnp.zeros_like(acc_ref)

    def gather(q, carry):
        left = []
        right = []
        for i in range(group):
            t = t_ref[q * group + i]
            r = r_ref[q * group + i]
            high = t // 256
            left.append(
                jnp.concatenate([r * jnp.where(high == h, 1.0, 0.0).astype(bf16) for h in range(highs)], axis=0)
            )
            low = t % 256
            rows = lax.broadcasted_iota(jnp.int32, (256, 256), 0)
            right.append(jnp.where(rows == low, 1.0, 0.0).astype(bf16))
        acc_ref[...] += lax.dot_general(
            jnp.concatenate(left, axis=1),
            jnp.concatenate(right, axis=1),
            (((1,), (1,)), ((), ())),
            preferred_element_type=f32,
        )
        return carry

    lax.fori_loop(0, n // 2 // group, gather, 0)

    for b in range(3 * nc):
        part = acc_ref[(b // 2) * R : (b // 2 + 1) * R, (b % 2) * BS : (b % 2 + 1) * BS]
        where = b // nc
        ref = (down_ref, mid_ref, up_ref)[where]
        ref[b - where * nc] = part.astype(ref.dtype)


def vmem():
    return pl.BlockSpec(memory_space=pltpu.VMEM)


def smem():
    return pl.BlockSpec(memory_space=pltpu.SMEM)


LIMIT = 16 * 1024 * 1024


def go_down(n, nc, near, f, g, t, f_edges, statics, so, weights):
    chunks = 4
    highs = 3 * nc // 2
    return pl.pallas_call(
        functools.partial(down_kernel, n, nc, so, chunks),
        out_shape=(
            jax.ShapeDtypeStruct((n, R, BS), f32),
            jax.ShapeDtypeStruct((nc, R, BS), bf16),
            jax.ShapeDtypeStruct((nc, R, BS), f32),
            jax.ShapeDtypeStruct((nc, R, BS), bf16),
        ),
        in_specs=[smem()] + [vmem()] * 7 + [pl.BlockSpec(memory_space=pl.ANY)],
        out_specs=(vmem(),) * 4,
        scratch_shapes=[
            pltpu.VMEM((n, K * BS, BS), bf16),
            pltpu.VMEM((n + 2 * EDGE, R, BS), bf16),
            pltpu.VMEM((n + EDGE, R, BS), bf16),
            pltpu.VMEM((n // 2, R, 2 * BS), bf16),
            pltpu.VMEM((highs * R, 2 * BS), f32),
            pltpu.SemaphoreType.DMA((chunks,)),
        ],
        compiler_params=pltpu.CompilerParams(vmem_limit_bytes=LIMIT),
        cost_estimate=pl.CostEstimate(
            flops=4 * n * R * K * BS * BS, transcendentals=0, bytes_accessed=n * K * BS * BS * 2
        ),
        name=f"down{n}",
    )(near, f, g, t, *f_edges, *statics, weights)


def prolong_kernel(n, nc, t_ref, lo_ref, own_ref, hi_ref, x_ref, out_ref, first_ref, last_ref, e_ref):
    highs = 3 * nc // 2
    for b in range(3 * nc):
        ref = (lo_ref, own_ref, hi_ref)[b // nc]
        e_ref[(b // 2) * R : (b // 2 + 1) * R, (b % 2) * BS : (b % 2 + 1) * BS] = ref[b % nc]

    def step(q, carry):
        t = t_ref[q]
        rows = lax.broadcasted_iota(jnp.int32, (256, 256), 0)
        pick = jnp.where(rows == t % 256, 1.0, 0.0).astype(bf16)
        found = jnp.dot(e_ref[...], pick, preferred_element_type=f32)
        high = t // 256
        y = jnp.zeros((R, 256), f32)
        for h in range(highs):
            y = y + jnp.where(high == h, found[h * R : (h + 1) * R], 0.0)
        out_ref[2 * q] = x_ref[2 * q] + y[:, :BS]
        out_ref[2 * q + 1] = x_ref[2 * q + 1] + y[:, BS:]
        return carry

    lax.fori_loop(0, n // 2, step, 0)
    first_ref[...] = out_ref[:EDGE].astype(bf16)
    last_ref[...] = out_ref[n - EDGE :].astype(bf16)


def prolong(n, nc, t, lo, own, hi, x):
    return pl.pallas_call(
        functools.partial(prolong_kernel, n, nc),
        out_shape=(
            jax.ShapeDtypeStruct((n, R, BS), f32),
            jax.ShapeDtypeStruct((EDGE, R, BS), bf16),
            jax.ShapeDtypeStruct((EDGE, R, BS), bf16),
        ),
        in_specs=[vmem()] * 5,
        out_specs=(vmem(),) * 3,
        scratch_shapes=[pltpu.VMEM((3 * nc // 2 * R, 2 * BS), bf16)],
        compiler_params=pltpu.CompilerParams(vmem_limit_bytes=LIMIT),
        cost_estimate=pl.CostEstimate(
            flops=2 * n * BS * 3 * nc * BS * R, transcendentals=0, bytes_accessed=2 * n * R * BS * 4
        ),
        name=f"prolong{n}",
    )(t, lo, own, hi, x)


def up_kernel(
    n, so, chunks,
    near_ref, x_ref, xlo_ref, xhi_ref, f_ref, g_ref, flo_ref, fhi_ref, slo_ref, shi_ref, w_hbm,
    out_ref,
    w_ref, v0_ref, v1_ref, keep_ref, sem,
):
    copies = load_weights(w_hbm, w_ref, sem, n, chunks)
    for c in copies:
        c.start()
    size = n // chunks

    def fill(b, carry):
        v0_ref[b + EDGE] = x_ref[b].astype(bf16)
        return carry

    lax.fori_loop(0, n, fill, 0, unroll=2)
    v0_ref[:EDGE] = xlo_ref[...]
    v0_ref[n + EDGE :] = xhi_ref[...]

    for side, fr, sr, xr in ((0, flo_ref, slo_ref, xlo_ref), (1, fhi_ref, shi_ref, xhi_ref)):
        for i in range(HB):
            e = i + HB * (1 - side)
            g = halo_diag(sr, so, e)
            s = jnp.where(g > 0, damping / g, 0.0)
            f = fr[e * R : (e + 1) * R, :].astype(f32)
            j = i + side * (n + HB)
            p = blocks_product(v0_ref, halo_weights(sr, so, i), near_ref, j, j)
            v1_ref[j] = (0.2 * xr[e].astype(f32) + s * (f + p)).astype(bf16)

    def sweep(b, x, p):
        s = damping / g_ref[pl.ds(b, 1), :]
        return 0.2 * x + s * (f_ref[b].astype(f32) + p)

    def first(b, carry):
        x = sweep(b, x_ref[b], blocks_product(v0_ref, w_ref[b], near_ref, b + HB, b + HB))
        keep_ref[b] = x
        v1_ref[b + HB] = x.astype(bf16)
        return carry

    for c in range(chunks):
        copies[c].wait()
        lax.fori_loop(c * size, (c + 1) * size, first, 0, unroll=4 if size % 4 == 0 else 2)

    def second(b, carry):
        p = blocks_product(v1_ref, w_ref[b], near_ref, b + HB, b)
        out_ref[b] = sweep(b, keep_ref[b], p).astype(out_ref.dtype)
        return carry

    lax.fori_loop(0, n, second, 0, unroll=4)


def go_up(n, near, x, x_edges, f, g, f_edges, statics, so, weights, dtype):
    chunks = 4
    return pl.pallas_call(
        functools.partial(up_kernel, n, so, chunks),
        out_shape=jax.ShapeDtypeStruct((n, R, BS), dtype),
        in_specs=[smem()] + [vmem()] * 9 + [pl.BlockSpec(memory_space=pl.ANY)],
        out_specs=vmem(),
        scratch_shapes=[
            pltpu.VMEM((n, K * BS, BS), bf16),
            pltpu.VMEM((n + 2 * EDGE, R, BS), bf16),
            pltpu.VMEM((n + EDGE, R, BS), bf16),
            pltpu.VMEM((n, R, BS), f32),
            pltpu.SemaphoreType.DMA((chunks,)),
        ],
        compiler_params=pltpu.CompilerParams(vmem_limit_bytes=LIMIT),
        cost_estimate=pl.CostEstimate(
            flops=4 * n * R * K * BS * BS, transcendentals=0, bytes_accessed=n * K * BS * BS * 2
        ),
        name=f"up{n}",
    )(near, x, *x_edges, f, g, *f_edges, *statics, weights)


def gather_rows(blocks):
    return jnp.transpose(blocks, (0, 2, 1)).reshape(-1, R)


def make_blocks(rows_data):
    return jnp.transpose(rows_data.reshape(-1, BS, R), (0, 2, 1))


def apply_operator(x, weights, near, degree):
    n = x.shape[0]
    rounded = x.astype(bf16)
    lo, hi = both_ways(rounded[n - HB :], rounded[:HB])
    extended = jnp.concatenate([lo, rounded, hi], axis=0)
    picked = extended[near + jnp.arange(n, dtype=jnp.int32)[:, None]]
    product = jnp.einsum("nkrb,nkbc->nrc", picked, weights, preferred_element_type=f32)
    return degree[:, None, :] * x - product / (K * BS)


def restrict(residual, targets, cc):
    partial = jax.ops.segment_sum(gather_rows(residual), targets.reshape(-1), num_segments=3 * cc)
    lo, hi = both_ways(partial[2 * cc :].astype(bf16), partial[:cc].astype(bf16))
    return partial[cc : 2 * cc] + lo + hi


def coarse_solve(coarse_rows, coarse_inverse):
    rounded = jnp.transpose(coarse_rows).astype(bf16)
    devices = lax.axis_size("col")
    got = lax.all_to_all(jnp.broadcast_to(rounded[None], (devices, *rounded.shape)), "col", 0, 0, tiled=True)
    got = jnp.moveaxis(got, 0, 1).reshape(R, -1)
    solved = lax.dot_general(got, coarse_inverse, (((1,), (1,)), ((), ())), preferred_element_type=f32)
    return jnp.transpose(solved)


def on_device(
    right_sides,
    weights_fine, columns_fine, degree_fine, owners_fine, slots_fine,
    weights_second, columns_second, degree_second, owners_second, slots_second,
    weights_third, columns_third, degree_third, owners_third, slots_third,
    coarse_inverse,
):
    device = lax.axis_index(AXES)

    def near_columns(columns):
        n = columns.shape[0]
        return columns - (device * n - HB + jnp.arange(n, dtype=jnp.int32)[:, None])

    def targets_of(owners, slots, cc):
        return (owners - device + 1) * cc + slots

    g1 = full_diagonal(weights_fine, degree_fine)
    g2 = full_diagonal(weights_second, degree_second)
    g3 = full_diagonal(weights_third, degree_third)
    near1, near2, near3 = near_columns(columns_fine), near_columns(columns_second), near_columns(columns_third)
    t1 = targets_of(owners_fine, slots_fine, NB1 * BS).reshape(NB0 // 2, 1, 2 * BS)
    t2 = targets_of(owners_second, slots_second, NB2 * BS).reshape(NB1 // 2, 1, 2 * BS)
    t3 = targets_of(owners_third, slots_third, C3)

    f = right_sides
    flat = lambda a: a.reshape(-1, BS)
    up1 = jnp.concatenate([flat(f[NB0 - EDGE :])] + edge_rows(weights_fine, g1, near1, False), axis=0)
    down1 = jnp.concatenate([flat(f[:EDGE])] + edge_rows(weights_fine, g1, near1, True), axis=0)
    e1 = both_ways(up1, down1)
    up2 = jnp.concatenate(edge_rows(weights_second, g2, near2, False), axis=0)
    down2 = jnp.concatenate(edge_rows(weights_second, g2, near2, True), axis=0)
    e2 = both_ways(up2, down2)
    fo = EDGE * R
    ext1 = jnp.concatenate([near_of(e1[0], fo), near1, near_of(e1[1], fo)], axis=0).reshape(-1)
    ext2 = jnp.concatenate([near_of(e2[0], 0), near2, near_of(e2[1], 0)], axis=0).reshape(-1)
    w1 = weights_fine.reshape(NB0, K * BS, BS)
    w2 = weights_second.reshape(NB1, K * BS, BS)

    x1, lower, middle, upper = go_down(NB0, NB1, ext1, f, g1, t1, e1, e1, fo, w1)
    lo, hi = both_ways(upper, lower)
    f2 = middle + lo.astype(f32) + hi.astype(f32)
    f2b = f2.astype(bf16)
    fe2 = both_ways(flat(f2b[NB1 - EDGE :]), flat(f2b[:EDGE]))
    x2, lower, middle, upper = go_down(NB1, NB2, ext2, f2, g2, t2, fe2, e2, 0, w2)
    lo, hi = both_ways(upper, lower)
    f3 = middle + lo.astype(f32) + hi.astype(f32)

    scale = g3[:, None, :]
    x3 = damping * f3 / scale
    x3 = x3 + damping * (f3 - apply_operator(x3, weights_third, near3, g3)) / scale
    residual = f3 - apply_operator(x3, weights_third, near3, g3)
    c = restrict(residual, t3, C3)
    u = coarse_solve(c, coarse_inverse).astype(bf16)
    lo, hi = both_ways(u, u)
    extended = jnp.concatenate([lo, u, hi], axis=0).astype(f32)
    x3 = x3 + make_blocks(extended[t3.reshape(-1)])
    for _ in range(2):
        x3 = x3 + damping * (f3 - apply_operator(x3, weights_third, near3, g3)) / scale

    x3 = x3.astype(bf16)
    lo, hi = both_ways(x3, x3)
    x2, first, last = prolong(NB1, NB2, t2, lo, x3, hi, x2)
    xe = both_ways(last, first)
    x2 = go_up(NB1, ext2, x2, xe, f2, g2, fe2, e2, 0, w2, bf16)
    lo, hi = both_ways(x2, x2)
    x1, first, last = prolong(NB0, NB1, t1, lo, x2, hi, x1)
    xe = both_ways(last, first)
    return go_up(NB0, ext1, x1, xe, f, g1, e1, e1, fo, w1, f32)


def solution(mesh):
    block = P(AXES, None, None)
    pair = P(AXES, None)
    four = P(AXES, None, None, None)
    level = (four, pair, pair, pair, pair)
    return jax.shard_map(
        on_device, mesh=mesh, in_specs=(block, *level, *level, *level, pair), out_specs=block, check_vma=False
    )
```

```python
import functools

import jax
import jax.numpy as jnp
from jax import lax
from jax.experimental import pallas as pl
from jax.experimental.pallas import tpu as pltpu
from jax.sharding import PartitionSpec as P

BS = 128
R = 64
K = 3
HB = 2
NB2 = 2
NB1 = 8
NB0 = 32
C3 = 128
AXES = ("row", "col")
EDGE = 2 * HB
ROWS = K * BS
damping = 0.8
bf16 = jnp.bfloat16
f32 = jnp.float32
i32 = jnp.int32
INV = 1.0 / (K * BS)

F_ROWS = EDGE * R
W_ROWS = HB * ROWS
TAIL = 16
EDGE1 = F_ROWS + W_ROWS + TAIL
EDGE2 = W_ROWS + TAIL
THIRD = NB2 * ROWS + TAIL
FIXED = EDGE2 + THIRD
FAR = NB2 * ROWS + 3 * TAIL


def passed_along(value, steps):
    count = lax.axis_size(AXES)
    return lax.ppermute(value, AXES, [(s, (s + steps) % count) for s in range(count)])


def both_ways(up, down, steps=1):
    return passed_along(up, steps), passed_along(down, -steps)


def in_hbm(x):
    return pltpu.with_memory_space_constraint(x, pltpu.HBM)


def vmem():
    return pl.BlockSpec(memory_space=pltpu.VMEM)


def smem():
    return pl.BlockSpec(memory_space=pltpu.SMEM)


def hbm():
    return pl.BlockSpec(memory_space=pltpu.HBM)


def shape(dims, dtype):
    return jax.ShapeDtypeStruct(dims, dtype)


def call(kernel, name, outs, in_specs, out_specs, scratch=(), mib=6, flops=0, nbytes=0):
    return pl.pallas_call(
        kernel,
        out_shape=outs,
        in_specs=in_specs,
        out_specs=out_specs,
        scratch_shapes=list(scratch),
        compiler_params=pltpu.CompilerParams(vmem_limit_bytes=mib * 1024 * 1024),
        cost_estimate=pl.CostEstimate(flops=flops, transcendentals=0, bytes_accessed=nbytes),
        name=name,
    )


def device_index():
    return lax.axis_index(AXES)


def near_row(values):
    lane = lax.broadcasted_iota(i32, (1, BS), 1)
    row = jnp.zeros((1, BS), f32)
    for i, v in enumerate(values):
        row = jnp.where(lane == i, v.astype(f32), row)
    return row


def read_near(row):
    lane = lax.broadcasted_iota(i32, (1, BS), 1)
    row = row.astype(f32)
    return [jnp.sum(jnp.where(lane == i, row, 0.0)).astype(i32) for i in range(HB * K)]


def near_of(col_ref, first, b, k):
    return col_ref[k, b] - (first + b - HB)


def column_sum(w):
    return jnp.sum(w.astype(f32), axis=0, keepdims=True)


def diagonal_rows(ref, at, stride, i):
    return ref[at + i : at + i + 1, :].astype(f32) + ref[at + stride + i : at + stride + i + 1, :].astype(f32)


def inverse(g):
    return jnp.where(g > 0, damping / g, 0.0)


def joined(v_ref, indices):
    return jnp.concatenate([v_ref[i] for i in indices], axis=1)


def product(v_ref, indices, w):
    return jnp.dot(joined(v_ref, indices), w, preferred_element_type=f32) * INV


def tail_rows(gs, nears, extra=()):
    high = [g.astype(bf16).astype(f32) for g in gs]
    low = [g - h for g, h in zip(gs, high)]
    rows = high + low + [near_row(nears)] + list(extra)
    rows = rows + [jnp.zeros((1, BS), f32)] * (TAIL - len(rows))
    return jnp.concatenate(rows, axis=0).astype(bf16)


def edge_kernel(f_hbm, w_hbm, deg_ref, col_ref, up_ref, down_ref, w_ref, sem):
    n = NB0
    first = device_index() * n
    copies = [
        pltpu.make_async_copy(w_hbm.at[pl.ds((n - EDGE) * ROWS, EDGE * ROWS)], w_ref.at[1], sem.at[0]),
        pltpu.make_async_copy(w_hbm.at[pl.ds(0, EDGE * ROWS)], w_ref.at[0], sem.at[1]),
        pltpu.make_async_copy(f_hbm.at[pl.ds((n - EDGE) * R, F_ROWS)], up_ref.at[pl.ds(0, F_ROWS)], sem.at[2]),
        pltpu.make_async_copy(f_hbm.at[pl.ds(0, F_ROWS)], down_ref.at[pl.ds(0, F_ROWS)], sem.at[3]),
        pltpu.make_async_copy(
            w_hbm.at[pl.ds((n - HB) * ROWS, W_ROWS)], up_ref.at[pl.ds(F_ROWS, W_ROWS)], sem.at[4]
        ),
        pltpu.make_async_copy(w_hbm.at[pl.ds(0, W_ROWS)], down_ref.at[pl.ds(F_ROWS, W_ROWS)], sem.at[5]),
    ]
    for c in copies:
        c.start()
    for side, ref, start, near_start in ((1, up_ref, n - EDGE, n - HB), (0, down_ref, 0, 0)):
        copies[1 - side].wait()
        gs = [
            deg_ref[start + i : start + i + 1, :] + column_sum(w_ref[side, i * ROWS : (i + 1) * ROWS, :]) * INV
            for i in range(EDGE)
        ]
        nears = [near_of(col_ref, first, near_start + i, k) for i in range(HB) for k in range(K)]
        ref[F_ROWS + W_ROWS :, :] = tail_rows(gs, nears)
    for c in copies[2:]:
        c.wait()


def first_edges(f, w, deg, col):
    return call(
        edge_kernel, "edges",
        (shape((EDGE1, BS), bf16),) * 2,
        [hbm(), hbm(), vmem(), smem()],
        (vmem(),) * 2,
        [pltpu.VMEM((2, EDGE * ROWS, BS), bf16), pltpu.SemaphoreType.DMA((6,))],
        flops=2**20, nbytes=2**21,
    )(f, w, deg, col)


def fixed_kernel(
    w1_hbm, w2_hbm, w3_hbm, deg1_ref, deg2_ref, deg3_ref, col2_ref, col3_ref, own3_ref, slot3_ref,
    g1_ref, g2_ref, g3_ref, up_ref, down_ref, w3_ref, tail_ref, w1_ref, w2_ref, sem,
):
    device = device_index()
    chunks = 4
    size = NB0 // chunks
    last3 = pltpu.make_async_copy(w3_hbm, w3_ref, sem.at[0])
    last2 = pltpu.make_async_copy(w2_hbm, w2_ref, sem.at[1])
    copies = [
        pltpu.make_async_copy(
            w2_hbm.at[pl.ds((NB1 - HB) * ROWS, W_ROWS)], up_ref.at[pl.ds(0, W_ROWS)], sem.at[2]
        ),
        pltpu.make_async_copy(w2_hbm.at[pl.ds(0, W_ROWS)], down_ref.at[pl.ds(0, W_ROWS)], sem.at[3]),
        pltpu.make_async_copy(w3_hbm, up_ref.at[pl.ds(EDGE2, W_ROWS)], sem.at[4]),
        pltpu.make_async_copy(w3_hbm, down_ref.at[pl.ds(EDGE2, W_ROWS)], sem.at[5]),
    ]
    bulk = [
        pltpu.make_async_copy(
            w1_hbm.at[pl.ds(c * size * ROWS, size * ROWS)], w1_ref.at[pl.ds(c * size * ROWS, size * ROWS)], sem.at[6 + c]
        )
        for c in range(chunks)
    ]
    for c in [last3, last2] + copies + bulk:
        c.start()
    last3.wait()
    g3 = [deg3_ref[i : i + 1, :] + column_sum(w3_ref[i * ROWS : (i + 1) * ROWS, :]) * INV for i in range(NB2)]
    for i in range(NB2):
        g3_ref[i : i + 1, :] = g3[i]
    nears = [near_of(col3_ref, device * NB2, i, k) for i in range(NB2) for k in range(K)]
    extra = [(own3_ref[i : i + 1, :] - device).astype(f32) for i in range(NB2)]
    extra = extra + [slot3_ref[i : i + 1, :].astype(f32) for i in range(NB2)]
    tail = tail_rows(g3, nears, extra)
    tail_ref[...] = tail
    up_ref[EDGE2 + W_ROWS :, :] = tail
    down_ref[EDGE2 + W_ROWS :, :] = tail
    last2.wait()
    g2 = [deg2_ref[i : i + 1, :] + column_sum(w2_ref[i * ROWS : (i + 1) * ROWS, :]) * INV for i in range(NB1)]
    for i in range(NB1):
        g2_ref[i : i + 1, :] = g2[i]
    first = device * NB1
    up_ref[W_ROWS : W_ROWS + TAIL, :] = tail_rows(
        g2[NB1 - EDGE :], [near_of(col2_ref, first, NB1 - HB + i, k) for i in range(HB) for k in range(K)]
    )
    down_ref[W_ROWS : W_ROWS + TAIL, :] = tail_rows(
        g2[:EDGE], [near_of(col2_ref, first, i, k) for i in range(HB) for k in range(K)]
    )

    def one(b, carry):
        at = pl.multiple_of(b * ROWS, ROWS)
        g1_ref[pl.ds(b, 1), :] = deg1_ref[pl.ds(b, 1), :] + column_sum(w1_ref[pl.ds(at, ROWS), :]) * INV
        return carry

    for c in range(chunks):
        bulk[c].wait()
        lax.fori_loop(c * size, (c + 1) * size, one, 0, unroll=2)
    for c in copies:
        c.wait()


def fixed_data(w1, w2, w3, deg1, deg2, deg3, col2, col3, own3, slot3):
    return call(
        fixed_kernel, "fixed",
        (
            shape((NB0, BS), f32), shape((NB1, BS), f32), shape((NB2, BS), f32),
            shape((FIXED, BS), bf16), shape((FIXED, BS), bf16),
            shape((NB2 * ROWS, BS), bf16), shape((TAIL, BS), bf16),
        ),
        [hbm()] * 3 + [vmem()] * 3 + [smem()] * 2 + [vmem()] * 2,
        (vmem(),) * 7,
        [
            pltpu.VMEM((NB0 * ROWS, BS), bf16),
            pltpu.VMEM((NB1 * ROWS, BS), bf16),
            pltpu.SemaphoreType.DMA((10,)),
        ],
        mib=10, flops=2**30, nbytes=2**22,
    )(w1, w2, w3, deg1, deg2, deg3, col2, col3, own3, slot3)


def far_kernel(w3_ref, tail_ref, lo_ref, hi_ref, out_ref):
    at = NB2 * ROWS
    out_ref[:at, :] = w3_ref[...]
    out_ref[at : at + TAIL, :] = lo_ref[FIXED - TAIL :, :]
    out_ref[at + TAIL : at + 2 * TAIL, :] = tail_ref[...]
    out_ref[at + 2 * TAIL :, :] = hi_ref[FIXED - TAIL :, :]


def far_data(w3, tail, lo, hi):
    return call(
        far_kernel, "far", shape((FAR, BS), bf16), [vmem()] * 4, vmem(), flops=2**20, nbytes=2**19
    )(w3, tail, lo, hi)


def weight_copies(w_hbm, w_ref, sem, n, chunks):
    size = n // chunks * ROWS
    return [
        pltpu.make_async_copy(w_hbm.at[pl.ds(c * size, size)], w_ref.at[pl.ds(c * size, size)], sem.at[c])
        for c in range(chunks)
    ]


def weight_of(w_ref, b):
    return w_ref[pl.ds(pl.multiple_of(b * ROWS, ROWS), ROWS), :]


def edge_starts(base, f_ref, s_ref):
    if base:
        rhs = lambda i: f_ref[i * R : (i + 1) * R, :].astype(f32)
    else:
        rhs = lambda i: f_ref[i].astype(f32)
    inv = [inverse(diagonal_rows(s_ref, base + W_ROWS, EDGE, i)) for i in range(EDGE)]
    return rhs, inv


def down_kernel(
    n, nc, base, chunks,
    col_ref, f_ref, g_ref, own_ref, slot_ref, flo_ref, fhi_ref, slo_ref, shi_ref, w_hbm,
    x_out, down_ref, mid_ref, up_ref,
    w_ref, v0_ref, v1_ref, x_ref, r_ref, acc_ref, sem,
):
    copies = weight_copies(w_hbm, w_ref, sem, n, chunks)
    for c in copies:
        c.start()
    size = n // chunks
    device = device_index()
    start = device * n

    def scale(b):
        return damping / g_ref[pl.ds(b, 1), :]

    def fill(b, carry):
        v0_ref[b + EDGE] = (f_ref[b].astype(f32) * scale(b)).astype(bf16)
        return carry

    lax.fori_loop(0, n, fill, 0, unroll=2)
    sides = []
    for side, fr, sr in ((0, flo_ref, slo_ref), (1, fhi_ref, shi_ref)):
        rhs, inv = edge_starts(base, fr, sr)
        starts = [rhs(i) * inv[i] for i in range(EDGE)]
        for i in range(EDGE):
            v0_ref[i + side * (n + EDGE)] = starts[i].astype(bf16)
        near = read_near(sr[base + W_ROWS + 2 * EDGE : base + W_ROWS + 2 * EDGE + 1, :])
        sides.append((side, sr, starts, inv, near))
    for side, sr, starts, inv, near in sides:
        for i in range(HB):
            e = i + HB * (1 - side)
            j = i + side * (n + HB)
            w = sr[base + i * ROWS : base + (i + 1) * ROWS, :]
            p = product(v0_ref, [j + near[i * K + k] for k in range(K)], w)
            v1_ref[j] = (1.2 * starts[e] + inv[e] * p).astype(bf16)

    def first(b, carry):
        p = product(v0_ref, [b + HB + near_of(col_ref, start, b, k) for k in range(K)], weight_of(w_ref, b))
        s = scale(b)
        x = 1.2 * (f_ref[b].astype(f32) * s) + s * p
        x_ref[b] = x
        v1_ref[b + HB] = x.astype(bf16)
        return carry

    for c in range(chunks):
        copies[c].wait()
        lax.fori_loop(c * size, (c + 1) * size, first, 0, unroll=4 if size % 4 == 0 else 2)
    saved = pltpu.make_async_copy(x_ref, x_out, sem.at[chunks])
    saved.start()

    def residual(b):
        p = product(v1_ref, [b + near_of(col_ref, start, b, k) for k in range(K)], weight_of(w_ref, b))
        return f_ref[b].astype(f32) - g_ref[pl.ds(b, 1), :] * x_ref[b] + p

    def second(q, carry):
        r_ref[q] = jnp.concatenate([residual(2 * q), residual(2 * q + 1)], axis=1).astype(bf16)
        return carry

    lax.fori_loop(0, n // 2, second, 0, unroll=2)

    highs = 3 * nc // 2
    group = 4
    acc_ref[...] = jnp.zeros_like(acc_ref)

    def gather(q, carry):
        left = []
        right = []
        for i in range(group):
            t = pair_targets(own_ref, slot_ref, device, nc, q * group + i)
            r = r_ref[q * group + i]
            high = t // 256
            left.append(
                jnp.concatenate([r * jnp.where(high == h, 1.0, 0.0).astype(bf16) for h in range(highs)], axis=0)
            )
            rows = lax.broadcasted_iota(i32, (256, 256), 0)
            right.append(jnp.where(rows == t % 256, 1.0, 0.0).astype(bf16))
        acc_ref[...] += lax.dot_general(
            jnp.concatenate(left, axis=1),
            jnp.concatenate(right, axis=1),
            (((1,), (1,)), ((), ())),
            preferred_element_type=f32,
        )
        return carry

    lax.fori_loop(0, n // 2 // group, gather, 0)

    for b in range(3 * nc):
        part = acc_ref[(b // 2) * R : (b // 2 + 1) * R, (b % 2) * BS : (b % 2 + 1) * BS]
        where = b // nc
        ref = (down_ref, mid_ref, up_ref)[where]
        ref[b - where * nc] = part.astype(ref.dtype)
    saved.wait()


def pair_targets(own_ref, slot_ref, device, nc, q):
    row = lambda b: (own_ref[pl.ds(b, 1), :] - device + 1) * (nc * BS) + slot_ref[pl.ds(b, 1), :]
    return jnp.concatenate([row(2 * q), row(2 * q + 1)], axis=1)


def go_down(n, nc, base, col, f, g, own, slot, f_edges, fixed, weights, mib):
    chunks = 4
    highs = 3 * nc // 2
    return call(
        functools.partial(down_kernel, n, nc, base, chunks), f"down{n}",
        (
            shape((n, R, BS), f32), shape((nc, R, BS), bf16), shape((nc, R, BS), f32), shape((nc, R, BS), bf16)
        ),
        [smem()] + [vmem()] * 8 + [hbm()],
        (hbm(), vmem(), vmem(), vmem()),
        [
            pltpu.VMEM((n * ROWS, BS), bf16),
            pltpu.VMEM((n + 2 * EDGE, R, BS), bf16),
            pltpu.VMEM((n + EDGE, R, BS), bf16),
            pltpu.VMEM((n, R, BS), f32),
            pltpu.VMEM((n // 2, R, 2 * BS), bf16),
            pltpu.VMEM((highs * R, 2 * BS), f32),
            pltpu.SemaphoreType.DMA((chunks + 1,)),
        ],
        mib=mib, flops=4 * n * R * ROWS * BS, nbytes=n * ROWS * BS * 2,
    )(col, f, g, own, slot, *f_edges, *fixed, weights)


def rhs_kernel(mid_ref, lo_ref, hi_ref, out_ref, up_ref, down_ref):
    out_ref[...] = mid_ref[...] + lo_ref[...].astype(f32) + hi_ref[...].astype(f32)
    up_ref[...] = out_ref[NB1 - EDGE :].astype(bf16)
    down_ref[...] = out_ref[:EDGE].astype(bf16)


def second_rhs(mid, lo, hi):
    return call(
        rhs_kernel, "rhs8",
        (shape((NB1, R, BS), f32), shape((EDGE, R, BS), bf16), shape((EDGE, R, BS), bf16)),
        [vmem()] * 3, (vmem(),) * 3, flops=2**18, nbytes=2**19,
    )(mid, lo, hi)


def spread(n, nc, e_ref, own_ref, slot_ref, device, x_ref, out_ref):
    highs = 3 * nc // 2

    def step(q, carry):
        t = pair_targets(own_ref, slot_ref, device, nc, q)
        rows = lax.broadcasted_iota(i32, (256, 256), 0)
        pick = jnp.where(rows == t % 256, 1.0, 0.0).astype(bf16)
        found = jnp.dot(e_ref[...], pick, preferred_element_type=f32)
        high = t // 256
        y = jnp.zeros((R, 256), f32)
        for h in range(highs):
            y = y + jnp.where(high == h, found[h * R : (h + 1) * R], 0.0)
        out_ref[2 * q] = x_ref[2 * q] + y[:, :BS]
        out_ref[2 * q + 1] = x_ref[2 * q + 1] + y[:, BS:]
        return carry

    lax.fori_loop(0, n // 2, step, 0)


def place(e_ref, b, value):
    e_ref[(b // 2) * R : (b // 2 + 1) * R, (b % 2) * BS : (b % 2 + 1) * BS] = value


def prolong_kernel(
    n, nc, own_ref, slot_ref, lo_ref, mid_ref, hi_ref, x_hbm, out_ref, first_ref, last_ref, e_ref, x_ref, sem
):
    copy = pltpu.make_async_copy(x_hbm, x_ref, sem.at[0])
    copy.start()
    for b in range(3 * nc):
        place(e_ref, b, (lo_ref, mid_ref, hi_ref)[b // nc][b % nc])
    copy.wait()
    spread(n, nc, e_ref, own_ref, slot_ref, device_index(), x_ref, out_ref)
    first_ref[...] = out_ref[:EDGE].astype(bf16)
    last_ref[...] = out_ref[n - EDGE :].astype(bf16)


def prolong(n, nc, own, slot, lo, mid, hi, x):
    return call(
        functools.partial(prolong_kernel, n, nc), f"prolong{n}",
        (shape((n, R, BS), f32), shape((EDGE, R, BS), bf16), shape((EDGE, R, BS), bf16)),
        [vmem()] * 5 + [hbm()],
        (vmem(),) * 3,
        [
            pltpu.VMEM((3 * nc // 2 * R, 2 * BS), bf16),
            pltpu.VMEM((n, R, BS), f32),
            pltpu.SemaphoreType.DMA((1,)),
        ],
        mib=12, flops=2 * n * BS * 3 * nc * BS * R, nbytes=2 * n * R * BS * 4,
    )(own, slot, lo, mid, hi, x)


def up_kernel(
    n, base, chunks,
    col_ref, x_ref, xlo_ref, xhi_ref, f_ref, g_ref, flo_ref, fhi_ref, slo_ref, shi_ref, w_hbm,
    out_ref,
    w_ref, v0_ref, v1_ref, keep_ref, sem,
):
    copies = weight_copies(w_hbm, w_ref, sem, n, chunks)
    for c in copies:
        c.start()
    size = n // chunks
    start = device_index() * n

    def fill(b, carry):
        v0_ref[b + EDGE] = x_ref[b].astype(bf16)
        return carry

    lax.fori_loop(0, n, fill, 0, unroll=2)
    v0_ref[:EDGE] = xlo_ref[...]
    v0_ref[n + EDGE :] = xhi_ref[...]
    sides = []
    for side, fr, sr, xr in ((0, flo_ref, slo_ref, xlo_ref), (1, fhi_ref, shi_ref, xhi_ref)):
        near = read_near(sr[base + W_ROWS + 2 * EDGE : base + W_ROWS + 2 * EDGE + 1, :])
        sides.append((side, sr, xr, *edge_starts(base, fr, sr), near))
    for side, sr, xr, rhs, inv, near in sides:
        for i in range(HB):
            e = i + HB * (1 - side)
            j = i + side * (n + HB)
            w = sr[base + i * ROWS : base + (i + 1) * ROWS, :]
            p = product(v0_ref, [j + near[i * K + k] for k in range(K)], w)
            v1_ref[j] = (0.2 * xr[e].astype(f32) + inv[e] * (rhs(e) + p)).astype(bf16)

    def sweep(b, x, p):
        return 0.2 * x + (damping / g_ref[pl.ds(b, 1), :]) * (f_ref[b].astype(f32) + p)

    def near(b, base):
        return [b + base + near_of(col_ref, start, b, k) for k in range(K)]

    def first(b, carry):
        x = sweep(b, x_ref[b], product(v0_ref, near(b, HB), weight_of(w_ref, b)))
        keep_ref[b] = x
        v1_ref[b + HB] = x.astype(bf16)
        return carry

    for c in range(chunks):
        copies[c].wait()
        lax.fori_loop(c * size, (c + 1) * size, first, 0, unroll=4 if size % 4 == 0 else 2)

    def second(b, carry):
        p = product(v1_ref, near(b, 0), weight_of(w_ref, b))
        out_ref[b] = sweep(b, keep_ref[b], p).astype(out_ref.dtype)
        return carry

    lax.fori_loop(0, n, second, 0, unroll=4)


def go_up(n, base, col, x, x_edges, f, g, f_edges, fixed, weights, dtype, mib):
    chunks = 4
    return call(
        functools.partial(up_kernel, n, base, chunks), f"up{n}",
        shape((n, R, BS), dtype),
        [smem()] + [vmem()] * 9 + [hbm()],
        vmem(),
        [
            pltpu.VMEM((n * ROWS, BS), bf16),
            pltpu.VMEM((n + 2 * EDGE, R, BS), bf16),
            pltpu.VMEM((n + EDGE, R, BS), bf16),
            pltpu.VMEM((n, R, BS), f32),
            pltpu.SemaphoreType.DMA((chunks,)),
        ],
        mib=mib, flops=4 * n * R * ROWS * BS, nbytes=n * ROWS * BS * 2,
    )(col, x, *x_edges, f, g, *f_edges, *fixed, weights)


def parts_kernel(low_ref, mid_ref, high_ref, out_ref):
    out_ref[:NB2] = low_ref[...]
    out_ref[NB2 : 2 * NB2] = mid_ref[...].astype(bf16)
    out_ref[2 * NB2 :] = high_ref[...]


def parts_of(low, mid, high):
    return call(
        parts_kernel, "parts", shape((3 * NB2, R, BS), bf16), [vmem()] * 3, vmem(), flops=2**17, nbytes=2**17
    )(low, mid, high)


def window_kernel(mid_ref, p_ref, lo_ref, hi_ref, f_ref, up_ref, down_ref):
    a, b = NB2, 2 * NB2
    f_ref[...] = mid_ref[...] + lo_ref[b:].astype(f32) + hi_ref[:a].astype(f32)
    own = f_ref[...].astype(bf16)
    up_ref[:a] = own
    up_ref[a:b] = (hi_ref[a:b].astype(f32) + p_ref[b:].astype(f32)).astype(bf16)
    up_ref[b:] = hi_ref[b:]
    down_ref[:a] = own
    down_ref[a:b] = (lo_ref[a:b].astype(f32) + p_ref[:a].astype(f32)).astype(bf16)
    down_ref[b:] = lo_ref[:a]


def third_window(mid, p, lo, hi):
    return call(
        window_kernel, "window",
        (shape((NB2, R, BS), f32), shape((3 * NB2, R, BS), bf16), shape((3 * NB2, R, BS), bf16)),
        [vmem()] * 4, (vmem(),) * 3, flops=2**18, nbytes=2**18,
    )(mid, p, lo, hi)


REACH = 3


def third_fixed(w3_ref, tail_ref, slo_ref, shi_ref, rlo_ref, rhi_ref):
    at = NB2 * ROWS
    tails = {0: (tail_ref, 0), -1: (slo_ref, FIXED - TAIL), 1: (shi_ref, FIXED - TAIL)}
    tails[-3], tails[-2] = (rlo_ref, at), (rlo_ref, at + TAIL)
    tails[2], tails[3] = (rhi_ref, at + TAIL), (rhi_ref, at + 2 * TAIL)
    matrices = {0: (w3_ref, 0), -1: (slo_ref, EDGE2), 1: (shi_ref, EDGE2), -2: (rlo_ref, 0), 2: (rhi_ref, 0)}
    diagonal = []
    for d in range(-REACH, REACH + 1):
        ref, at = tails[d]
        diagonal += [diagonal_rows(ref, at, NB2, i) for i in range(NB2)]
    near = {}
    for d in range(-2, 3):
        ref, at = tails[d]
        near[d] = read_near(ref[at + 2 * NB2 : at + 2 * NB2 + 1, :])

    def weights(j):
        ref, at = matrices[j // NB2 - 2]
        return ref[at + (j % NB2) * ROWS : at + (j % NB2 + 1) * ROWS, :]

    def columns(j):
        return near[j // NB2 - 2][(j % NB2) * K : (j % NB2 + 1) * K]

    def row(d, kind):
        ref, at = tails[d]
        at = at + 2 * NB2 + 1 + kind * NB2
        return jnp.concatenate([ref[at + i : at + i + 1, :] for i in range(NB2)], axis=1).astype(f32).astype(i32)

    return diagonal, weights, columns, row


def third_down_kernel(
    f_ref, p_ref, lo_ref, hi_ref, dlo_ref, dhi_ref, w3_ref, tail_ref, slo_ref, shi_ref, rlo_ref, rhi_ref,
    c_ref, z_ref,
    v0_ref, v1_ref, v2_ref,
):
    diagonal, weights, columns, row = third_fixed(w3_ref, tail_ref, slo_ref, shi_ref, rlo_ref, rhi_ref)
    a, b = NB2, 2 * NB2
    wide = lambda ref, s, i: ref[s + i].astype(f32)
    f = []
    f += [wide(dlo_ref, 0, i) for i in range(a)]
    f += [wide(dlo_ref, a, i) + wide(lo_ref, 0, i) for i in range(a)]
    f += [wide(dlo_ref, b, i) + wide(lo_ref, a, i) + wide(p_ref, 0, i) for i in range(a)]
    f += [f_ref[i] for i in range(a)]
    f += [wide(dhi_ref, b, i) + wide(hi_ref, a, i) + wide(p_ref, b, i) for i in range(a)]
    f += [wide(dhi_ref, a, i) + wide(hi_ref, b, i) for i in range(a)]
    f += [wide(dhi_ref, 0, i) for i in range(a)]
    count = len(f)
    inv = [damping / g for g in diagonal]
    start = [f[i] * inv[i] for i in range(count)]
    for i in range(count):
        v0_ref[i] = start[i].astype(bf16)
    x1 = []
    for j in range(count - 4):
        p = product(v0_ref, [j + c for c in columns(j)], weights(j))
        x1.append(1.2 * start[j + 2] + inv[j + 2] * p)
        v1_ref[j] = x1[j].astype(bf16)
    res = []
    x2 = []
    for j in range(count - 8):
        p = product(v1_ref, [j + c for c in columns(j + 2)], weights(j + 2))
        r = f[j + 4] - diagonal[j + 4] * x1[j + 2] + p
        res.append(r)
        x2.append(x1[j + 2] + inv[j + 4] * r)
        v2_ref[j] = x2[j].astype(bf16)
    left = []
    right = []
    for d in (-1, 0, 1):
        r = jnp.concatenate(res[(d + 1) * a : (d + 2) * a], axis=1)
        left.append(jnp.where(row(d, 0) == -d, r, 0.0).astype(bf16))
        rows = lax.broadcasted_iota(i32, (C3, NB2 * BS), 0)
        right.append(jnp.where(rows == row(d, 1), 1.0, 0.0).astype(bf16))
    c = lax.dot_general(
        jnp.concatenate(left, axis=1), jnp.concatenate(right, axis=1),
        (((1,), (1,)), ((), ())), preferred_element_type=f32,
    ).astype(bf16)
    for i in range(c_ref.shape[0]):
        c_ref[i] = c
    for i in range(a):
        p = product(v2_ref, [i + c for c in columns(i + 4)], weights(i + 4))
        z_ref[i] = 0.2 * x2[i + 2] + start[i + 6] + inv[i + 6] * p


def third_down(copies, *args):
    count = 2 * NB2 * REACH + NB2
    return call(
        third_down_kernel, "down2",
        (shape((copies, R, C3), bf16), shape((NB2, R, BS), f32)),
        [vmem()] * 12, (vmem(),) * 2,
        [
            pltpu.VMEM((count, R, BS), bf16), pltpu.VMEM((count - 4, R, BS), bf16), pltpu.VMEM((count - 8, R, BS), bf16)
        ],
        mib=12, flops=2**27, nbytes=2**21,
    )(*args)


def coarse_kernel(got_ref, z_ref, s_hbm, out_ref, s_ref, sem):
    count = got_ref.shape[0]
    chunks = 4
    size = count // chunks
    copies = [
        pltpu.make_async_copy(s_hbm.at[:, pl.ds(c * size * BS, size * BS)], s_ref.at[c], sem.at[c])
        for c in range(chunks)
    ]
    for c in copies:
        c.start()
    u = jnp.zeros((R, C3), f32)
    for c in range(chunks):
        copies[c].wait()
        u = u + lax.dot_general(
            joined(got_ref, range(c * size, (c + 1) * size)), s_ref[c],
            (((1,), (1,)), ((), ())), preferred_element_type=f32,
        )
    out_ref[0] = u.astype(bf16)
    out_ref[1:] = z_ref[...].astype(bf16)


def coarse_solve(got, z, inverse_rows):
    count = got.shape[0]
    return call(
        coarse_kernel, "coarse", shape((1 + NB2, R, BS), bf16),
        [vmem(), vmem(), hbm()], vmem(),
        [pltpu.VMEM((4, C3, count // 4 * BS), bf16), pltpu.SemaphoreType.DMA((4,))],
        flops=2**26, nbytes=2**21,
    )(got, z, inverse_rows)


def three_kernel(lo_ref, own_ref, hi_ref, out_ref):
    out_ref[0] = lo_ref[0]
    out_ref[1] = own_ref[0]
    out_ref[2] = hi_ref[0]


def three_of(lo, own, hi):
    return call(
        three_kernel, "three", shape((3, R, BS), bf16), [vmem()] * 3, vmem(), flops=2**15, nbytes=2**16
    )(lo, own, hi)


def third_up_kernel(
    own_ref, lo_ref, hi_ref, ulo_ref, uhi_ref, z_ref, w3_ref, tail_ref, slo_ref, shi_ref, rlo_ref, rhi_ref,
    own2_ref, slot2_ref, x_hbm,
    out_ref, first_ref, last_ref,
    v0_ref, v1_ref, e_ref, x_ref, sem,
):
    copy = pltpu.make_async_copy(x_hbm, x_ref, sem.at[0])
    copy.start()
    diagonal, weights, columns, row = third_fixed(w3_ref, tail_ref, slo_ref, shi_ref, rlo_ref, rhi_ref)
    inv = [damping / g for g in diagonal]
    u = [ulo_ref[0], ulo_ref[1], ulo_ref[2], lo_ref[0], own_ref[0], hi_ref[0], uhi_ref[0], uhi_ref[1], uhi_ref[2]]
    y = []
    for d in range(-REACH, REACH + 1):
        rows = lax.broadcasted_iota(i32, (C3, NB2 * BS), 0)
        pick = jnp.where(rows == row(d, 1), 1.0, 0.0).astype(bf16)
        at = d + REACH
        found = jnp.dot(jnp.concatenate(u[at : at + 3], axis=0), pick, preferred_element_type=f32)
        owner = row(d, 0)
        got = jnp.zeros((R, NB2 * BS), f32)
        for i in range(3):
            got = got + jnp.where(owner == i - 1, found[i * R : (i + 1) * R], 0.0)
        y += [got[:, i * BS : (i + 1) * BS] for i in range(NB2)]
    count = len(y)
    for i in range(count):
        v0_ref[i] = y[i].astype(bf16)
    y1 = []
    for j in range(count - 4):
        p = product(v0_ref, [j + c for c in columns(j)], weights(j))
        y1.append(0.2 * y[j + 2] + inv[j + 2] * p)
        v1_ref[j] = y1[j].astype(bf16)
    for j in range(count - 8):
        p = product(v1_ref, [j + c for c in columns(j + 2)], weights(j + 2))
        y2 = 0.2 * y1[j + 2] + inv[j + 4] * p
        i = j % NB2
        z = (lambda: lo_ref[1 + i].astype(f32), lambda: z_ref[i], lambda: hi_ref[1 + i].astype(f32))[j // NB2]()
        place(e_ref, j, (z + y2).astype(bf16))
    copy.wait()
    spread(NB1, NB2, e_ref, own2_ref, slot2_ref, device_index(), x_ref, out_ref)
    first_ref[...] = out_ref[:EDGE].astype(bf16)
    last_ref[...] = out_ref[NB1 - EDGE :].astype(bf16)


def third_up(*args):
    count = 2 * NB2 * REACH + NB2
    return call(
        third_up_kernel, "up2",
        (shape((NB1, R, BS), f32), shape((EDGE, R, BS), bf16), shape((EDGE, R, BS), bf16)),
        [vmem()] * 14 + [hbm()], (vmem(),) * 3,
        [
            pltpu.VMEM((count, R, BS), bf16), pltpu.VMEM((count - 4, R, BS), bf16),
            pltpu.VMEM((3 * NB2 // 2 * R, 2 * BS), bf16), pltpu.VMEM((NB1, R, BS), f32),
            pltpu.SemaphoreType.DMA((1,)),
        ],
        mib=12, flops=2**27, nbytes=2**21,
    )(*args)


def on_device(
    right_sides,
    weights_fine, columns_fine, degree_fine, owners_fine, slots_fine,
    weights_second, columns_second, degree_second, owners_second, slots_second,
    weights_third, columns_third, degree_third, owners_third, slots_third,
    coarse_inverse,
):
    flat = lambda a: a.reshape(-1, BS)
    f = right_sides
    columns_fine, columns_second, columns_third = columns_fine.T, columns_second.T, columns_third.T
    w1, w2, w3 = (in_hbm(flat(w)) for w in (weights_fine, weights_second, weights_third))
    coarse_inverse = in_hbm(coarse_inverse)
    edges1 = both_ways(*first_edges(in_hbm(flat(f)), w1, degree_fine, columns_fine))
    g1, g2, _, up, down, w3, tail = fixed_data(
        w1, w2, w3, degree_fine, degree_second, degree_third, columns_second, columns_third, owners_third, slots_third
    )
    fixed = both_ways(up, down)
    far = far_data(w3, tail, *fixed)
    far = both_ways(far, far, 2)
    third = (w3, tail, *fixed, *far)

    x1, low, mid, high = go_down(
        NB0, NB1, F_ROWS, columns_fine, f, g1, owners_fine, slots_fine, edges1, edges1, w1, 20
    )
    lo, hi = both_ways(high, low)
    f2, up, down = second_rhs(mid, lo, hi)
    f_edges = both_ways(up, down)
    x2, low, mid, high = go_down(
        NB1, NB2, 0, columns_second, f2, g2, owners_second, slots_second, f_edges, fixed, w2, 12
    )
    parts = parts_of(low, mid, high)
    plo, phi = both_ways(parts, parts)
    f3, up, down = third_window(mid, parts, plo, phi)
    dlo, dhi = both_ways(up, down, 3)
    c, z = third_down(lax.axis_size("col"), f3, parts, plo, phi, dlo, dhi, *third)
    got = lax.all_to_all(c, "col", 0, 0, tiled=True)
    own = coarse_solve(got, z, coarse_inverse)
    lo, hi = both_ways(own, own)
    near = three_of(lo, own, hi)
    ulo, uhi = both_ways(near, near, 3)
    x2, first, last = third_up(own, lo, hi, ulo, uhi, z, *third, owners_second, slots_second, x2)
    x_edges = both_ways(last, first)
    x2 = go_up(NB1, 0, columns_second, x2, x_edges, f2, g2, f_edges, fixed, w2, bf16, 12)
    lo, hi = both_ways(x2, x2)
    x1, first, last = prolong(NB0, NB1, owners_fine, slots_fine, lo, x2, hi, x1)
    x_edges = both_ways(last, first)
    return go_up(NB0, F_ROWS, columns_fine, x1, x_edges, f, g1, edges1, edges1, w1, f32, 20)


def solution(mesh):
    block = P(AXES, None, None)
    pair = P(AXES, None)
    four = P(AXES, None, None, None)
    level = (four, pair, pair, pair, pair)
    return jax.shard_map(
        on_device, mesh=mesh, in_specs=(block, *level, *level, *level, pair), out_specs=block, check_vma=False
    )
```

```python
import functools

import jax
import jax.numpy as jnp
from jax import lax
from jax.experimental import pallas as pl
from jax.experimental.pallas import tpu as pltpu
from jax.sharding import PartitionSpec as P

BS = 128
R = 64
K = 3
HB = 2
NB2 = 2
NB1 = 8
NB0 = 32
C3 = 128
AXES = ("row", "col")
EDGE = 2 * HB
ROWS = K * BS
damping = 0.8
bf16 = jnp.bfloat16
f32 = jnp.float32
i32 = jnp.int32
INV = 1.0 / (K * BS)

F_ROWS = EDGE * R
W_ROWS = HB * ROWS
TAIL = 16
EDGE1 = F_ROWS + W_ROWS + TAIL
EDGE2 = W_ROWS + TAIL
THIRD = NB2 * ROWS + TAIL
FIXED = EDGE2 + THIRD
FAR = NB2 * ROWS + 3 * TAIL


def passed_along(value, steps):
    count = lax.axis_size(AXES)
    return lax.ppermute(value, AXES, [(s, (s + steps) % count) for s in range(count)])


def both_ways(up, down, steps=1):
    return passed_along(up, steps), passed_along(down, -steps)


def in_hbm(x):
    return pltpu.with_memory_space_constraint(x, pltpu.HBM)


def vmem():
    return pl.BlockSpec(memory_space=pltpu.VMEM)


def smem():
    return pl.BlockSpec(memory_space=pltpu.SMEM)


def hbm():
    return pl.BlockSpec(memory_space=pltpu.HBM)


def shape(dims, dtype):
    return jax.ShapeDtypeStruct(dims, dtype)


def call(kernel, name, outs, in_specs, out_specs, scratch=(), mib=6, flops=0, nbytes=0):
    return pl.pallas_call(
        kernel,
        out_shape=outs,
        in_specs=in_specs,
        out_specs=out_specs,
        scratch_shapes=list(scratch),
        compiler_params=pltpu.CompilerParams(vmem_limit_bytes=mib * 1024 * 1024),
        cost_estimate=pl.CostEstimate(flops=flops, transcendentals=0, bytes_accessed=nbytes),
        name=name,
    )


def device_index():
    return lax.axis_index(AXES)


def near_row(values):
    lane = lax.broadcasted_iota(i32, (1, BS), 1)
    row = jnp.zeros((1, BS), f32)
    for i, v in enumerate(values):
        row = jnp.where(lane == i, v.astype(f32), row)
    return row


def read_near(row):
    lane = lax.broadcasted_iota(i32, (1, BS), 1)
    row = row.astype(f32)
    return [jnp.sum(jnp.where(lane == i, row, 0.0)).astype(i32) for i in range(HB * K)]


def near_of(col_ref, first, b, k):
    return col_ref[k, b] - (first + b - HB)


def column_sum(w):
    return jnp.sum(w.astype(f32), axis=0, keepdims=True)


def diagonal_rows(ref, at, stride, i):
    return ref[at + i : at + i + 1, :].astype(f32) + ref[at + stride + i : at + stride + i + 1, :].astype(f32)


def inverse(g):
    return jnp.where(g > 0, damping / g, 0.0)


def joined(v_ref, indices):
    return jnp.concatenate([v_ref[i] for i in indices], axis=1)


def product(v_ref, indices, w):
    return jnp.dot(joined(v_ref, indices), w, preferred_element_type=f32) * INV


def tail_rows(gs, nears, extra=()):
    high = [g.astype(bf16).astype(f32) for g in gs]
    low = [g - h for g, h in zip(gs, high)]
    rows = high + low + [near_row(nears)] + list(extra)
    rows = rows + [jnp.zeros((1, BS), f32)] * (TAIL - len(rows))
    return jnp.concatenate(rows, axis=0).astype(bf16)


def edge_kernel(f_hbm, w_hbm, deg_ref, col_ref, up_ref, down_ref, w_ref, sem):
    n = NB0
    first = device_index() * n
    copies = [
        pltpu.make_async_copy(w_hbm.at[pl.ds((n - EDGE) * ROWS, EDGE * ROWS)], w_ref.at[1], sem.at[0]),
        pltpu.make_async_copy(w_hbm.at[pl.ds(0, EDGE * ROWS)], w_ref.at[0], sem.at[1]),
        pltpu.make_async_copy(f_hbm.at[pl.ds((n - EDGE) * R, F_ROWS)], up_ref.at[pl.ds(0, F_ROWS)], sem.at[2]),
        pltpu.make_async_copy(f_hbm.at[pl.ds(0, F_ROWS)], down_ref.at[pl.ds(0, F_ROWS)], sem.at[3]),
        pltpu.make_async_copy(
            w_hbm.at[pl.ds((n - HB) * ROWS, W_ROWS)], up_ref.at[pl.ds(F_ROWS, W_ROWS)], sem.at[4]
        ),
        pltpu.make_async_copy(w_hbm.at[pl.ds(0, W_ROWS)], down_ref.at[pl.ds(F_ROWS, W_ROWS)], sem.at[5]),
    ]
    for c in copies:
        c.start()
    for side, ref, start, near_start in ((1, up_ref, n - EDGE, n - HB), (0, down_ref, 0, 0)):
        copies[1 - side].wait()
        gs = [
            deg_ref[start + i : start + i + 1, :] + column_sum(w_ref[side, i * ROWS : (i + 1) * ROWS, :]) * INV
            for i in range(EDGE)
        ]
        nears = [near_of(col_ref, first, near_start + i, k) for i in range(HB) for k in range(K)]
        ref[F_ROWS + W_ROWS :, :] = tail_rows(gs, nears)
    for c in copies[2:]:
        c.wait()


def first_edges(f, w, deg, col):
    return call(
        edge_kernel, "edges",
        (shape((EDGE1, BS), bf16),) * 2,
        [hbm(), hbm(), vmem(), smem()],
        (vmem(),) * 2,
        [pltpu.VMEM((2, EDGE * ROWS, BS), bf16), pltpu.SemaphoreType.DMA((6,))],
        flops=2**20, nbytes=2**21,
    )(f, w, deg, col)


def fixed_kernel(
    w1_hbm, w2_hbm, w3_hbm, deg1_ref, deg2_ref, deg3_ref, col2_ref, col3_ref, own3_ref, slot3_ref,
    g1_ref, g2_ref, g3_ref, up_ref, down_ref, w3_ref, tail_ref, w1_ref, w2_ref, sem,
):
    device = device_index()
    chunks = 4
    size = NB0 // chunks
    last3 = pltpu.make_async_copy(w3_hbm, w3_ref, sem.at[0])
    last2 = pltpu.make_async_copy(w2_hbm, w2_ref, sem.at[1])
    copies = [
        pltpu.make_async_copy(
            w2_hbm.at[pl.ds((NB1 - HB) * ROWS, W_ROWS)], up_ref.at[pl.ds(0, W_ROWS)], sem.at[2]
        ),
        pltpu.make_async_copy(w2_hbm.at[pl.ds(0, W_ROWS)], down_ref.at[pl.ds(0, W_ROWS)], sem.at[3]),
        pltpu.make_async_copy(w3_hbm, up_ref.at[pl.ds(EDGE2, W_ROWS)], sem.at[4]),
        pltpu.make_async_copy(w3_hbm, down_ref.at[pl.ds(EDGE2, W_ROWS)], sem.at[5]),
    ]
    bulk = [
        pltpu.make_async_copy(
            w1_hbm.at[pl.ds(c * size * ROWS, size * ROWS)], w1_ref.at[pl.ds(c * size * ROWS, size * ROWS)], sem.at[6 + c]
        )
        for c in range(chunks)
    ]
    for c in [last3, last2] + copies + bulk:
        c.start()
    last3.wait()
    g3 = [deg3_ref[i : i + 1, :] + column_sum(w3_ref[i * ROWS : (i + 1) * ROWS, :]) * INV for i in range(NB2)]
    for i in range(NB2):
        g3_ref[i : i + 1, :] = g3[i]
    nears = [near_of(col3_ref, device * NB2, i, k) for i in range(NB2) for k in range(K)]
    extra = [(own3_ref[i : i + 1, :] - device).astype(f32) for i in range(NB2)]
    extra = extra + [slot3_ref[i : i + 1, :].astype(f32) for i in range(NB2)]
    tail = tail_rows(g3, nears, extra)
    tail_ref[...] = tail
    up_ref[EDGE2 + W_ROWS :, :] = tail
    down_ref[EDGE2 + W_ROWS :, :] = tail
    last2.wait()
    g2 = [deg2_ref[i : i + 1, :] + column_sum(w2_ref[i * ROWS : (i + 1) * ROWS, :]) * INV for i in range(NB1)]
    for i in range(NB1):
        g2_ref[i : i + 1, :] = g2[i]
    first = device * NB1
    up_ref[W_ROWS : W_ROWS + TAIL, :] = tail_rows(
        g2[NB1 - EDGE :], [near_of(col2_ref, first, NB1 - HB + i, k) for i in range(HB) for k in range(K)]
    )
    down_ref[W_ROWS : W_ROWS + TAIL, :] = tail_rows(
        g2[:EDGE], [near_of(col2_ref, first, i, k) for i in range(HB) for k in range(K)]
    )

    def one(b, carry):
        at = pl.multiple_of(b * ROWS, ROWS)
        g1_ref[pl.ds(b, 1), :] = deg1_ref[pl.ds(b, 1), :] + column_sum(w1_ref[pl.ds(at, ROWS), :]) * INV
        return carry

    for c in range(chunks):
        bulk[c].wait()
        lax.fori_loop(c * size, (c + 1) * size, one, 0, unroll=2)
    for c in copies:
        c.wait()


def fixed_data(w1, w2, w3, deg1, deg2, deg3, col2, col3, own3, slot3):
    return call(
        fixed_kernel, "fixed",
        (
            shape((NB0, BS), f32), shape((NB1, BS), f32), shape((NB2, BS), f32),
            shape((FIXED, BS), bf16), shape((FIXED, BS), bf16),
            shape((NB2 * ROWS, BS), bf16), shape((TAIL, BS), bf16),
        ),
        [hbm()] * 3 + [vmem()] * 3 + [smem()] * 2 + [vmem()] * 2,
        (vmem(),) * 7,
        [
            pltpu.VMEM((NB0 * ROWS, BS), bf16),
            pltpu.VMEM((NB1 * ROWS, BS), bf16),
            pltpu.SemaphoreType.DMA((10,)),
        ],
        mib=10, flops=2**30, nbytes=2**22,
    )(w1, w2, w3, deg1, deg2, deg3, col2, col3, own3, slot3)


def far_kernel(w3_ref, tail_ref, lo_ref, hi_ref, out_ref, copy_ref):
    at = NB2 * ROWS
    out_ref[:at, :] = w3_ref[...]
    out_ref[at : at + TAIL, :] = lo_ref[FIXED - TAIL :, :]
    out_ref[at + TAIL : at + 2 * TAIL, :] = tail_ref[...]
    out_ref[at + 2 * TAIL :, :] = hi_ref[FIXED - TAIL :, :]
    copy_ref[...] = out_ref[...]


def far_data(w3, tail, lo, hi):
    return call(
        far_kernel, "far", (shape((FAR, BS), bf16),) * 2, [vmem()] * 4, (vmem(),) * 2, flops=2**20, nbytes=2**19
    )(w3, tail, lo, hi)


def weight_copies(w_hbm, w_ref, sem, n, chunks):
    size = n // chunks * ROWS
    return [
        pltpu.make_async_copy(w_hbm.at[pl.ds(c * size, size)], w_ref.at[pl.ds(c * size, size)], sem.at[c])
        for c in range(chunks)
    ]


def weight_of(w_ref, b):
    return w_ref[pl.ds(pl.multiple_of(b * ROWS, ROWS), ROWS), :]


def edge_starts(base, f_ref, s_ref):
    if base:
        rhs = lambda i: f_ref[i * R : (i + 1) * R, :].astype(f32)
    else:
        rhs = lambda i: f_ref[i].astype(f32)
    inv = [inverse(diagonal_rows(s_ref, base + W_ROWS, EDGE, i)) for i in range(EDGE)]
    return rhs, inv


def down_kernel(
    n, nc, base, chunks,
    col_ref, f_ref, g_ref, own_ref, slot_ref, flo_ref, fhi_ref, slo_ref, shi_ref, w_hbm,
    x_out, down_ref, mid_ref, up_ref,
    w_ref, v0_ref, v1_ref, x_ref, r_ref, acc_ref, sem,
):
    copies = weight_copies(w_hbm, w_ref, sem, n, chunks)
    for c in copies:
        c.start()
    size = n // chunks
    device = device_index()
    start = device * n

    def scale(b):
        return damping / g_ref[pl.ds(b, 1), :]

    def fill(b, carry):
        v0_ref[b + EDGE] = (f_ref[b].astype(f32) * scale(b)).astype(bf16)
        return carry

    lax.fori_loop(0, n, fill, 0, unroll=2)
    sides = []
    for side, fr, sr in ((0, flo_ref, slo_ref), (1, fhi_ref, shi_ref)):
        rhs, inv = edge_starts(base, fr, sr)
        starts = [rhs(i) * inv[i] for i in range(EDGE)]
        for i in range(EDGE):
            v0_ref[i + side * (n + EDGE)] = starts[i].astype(bf16)
        near = read_near(sr[base + W_ROWS + 2 * EDGE : base + W_ROWS + 2 * EDGE + 1, :])
        sides.append((side, sr, starts, inv, near))
    for side, sr, starts, inv, near in sides:
        for i in range(HB):
            e = i + HB * (1 - side)
            j = i + side * (n + HB)
            w = sr[base + i * ROWS : base + (i + 1) * ROWS, :]
            p = product(v0_ref, [j + near[i * K + k] for k in range(K)], w)
            v1_ref[j] = (1.2 * starts[e] + inv[e] * p).astype(bf16)

    def first(b, carry):
        p = product(v0_ref, [b + HB + near_of(col_ref, start, b, k) for k in range(K)], weight_of(w_ref, b))
        s = scale(b)
        x = 1.2 * (f_ref[b].astype(f32) * s) + s * p
        x_ref[b] = x
        v1_ref[b + HB] = x.astype(bf16)
        return carry

    for c in range(chunks):
        copies[c].wait()
        lax.fori_loop(c * size, (c + 1) * size, first, 0, unroll=4 if size % 4 == 0 else 2)
    saved = pltpu.make_async_copy(x_ref, x_out, sem.at[chunks])
    saved.start()

    def residual(b):
        p = product(v1_ref, [b + near_of(col_ref, start, b, k) for k in range(K)], weight_of(w_ref, b))
        return f_ref[b].astype(f32) - g_ref[pl.ds(b, 1), :] * x_ref[b] + p

    def second(q, carry):
        r_ref[q] = jnp.concatenate([residual(2 * q), residual(2 * q + 1)], axis=1).astype(bf16)
        return carry

    lax.fori_loop(0, n // 2, second, 0, unroll=2)

    highs = 3 * nc // 2
    group = 4
    acc_ref[...] = jnp.zeros_like(acc_ref)

    def gather(q, carry):
        left = []
        right = []
        for i in range(group):
            t = pair_targets(own_ref, slot_ref, device, nc, q * group + i)
            r = r_ref[q * group + i]
            high = t // 256
            left.append(
                jnp.concatenate([r * jnp.where(high == h, 1.0, 0.0).astype(bf16) for h in range(highs)], axis=0)
            )
            rows = lax.broadcasted_iota(i32, (256, 256), 0)
            right.append(jnp.where(rows == t % 256, 1.0, 0.0).astype(bf16))
        acc_ref[...] += lax.dot_general(
            jnp.concatenate(left, axis=1),
            jnp.concatenate(right, axis=1),
            (((1,), (1,)), ((), ())),
            preferred_element_type=f32,
        )
        return carry

    lax.fori_loop(0, n // 2 // group, gather, 0)

    for b in range(3 * nc):
        part = acc_ref[(b // 2) * R : (b // 2 + 1) * R, (b % 2) * BS : (b % 2 + 1) * BS]
        where = b // nc
        ref = (down_ref, mid_ref, up_ref)[where]
        ref[b - where * nc] = part.astype(ref.dtype)
    saved.wait()


def pair_targets(own_ref, slot_ref, device, nc, q):
    row = lambda b: (own_ref[pl.ds(b, 1), :] - device + 1) * (nc * BS) + slot_ref[pl.ds(b, 1), :]
    return jnp.concatenate([row(2 * q), row(2 * q + 1)], axis=1)


def go_down(n, nc, base, col, f, g, own, slot, f_edges, fixed, weights, mib):
    chunks = 4
    highs = 3 * nc // 2
    return call(
        functools.partial(down_kernel, n, nc, base, chunks), f"down{n}",
        (
            shape((n, R, BS), f32), shape((nc, R, BS), bf16), shape((nc, R, BS), f32), shape((nc, R, BS), bf16)
        ),
        [smem()] + [vmem()] * 8 + [hbm()],
        (hbm(), vmem(), vmem(), vmem()),
        [
            pltpu.VMEM((n * ROWS, BS), bf16),
            pltpu.VMEM((n + 2 * EDGE, R, BS), bf16),
            pltpu.VMEM((n + EDGE, R, BS), bf16),
            pltpu.VMEM((n, R, BS), f32),
            pltpu.VMEM((n // 2, R, 2 * BS), bf16),
            pltpu.VMEM((highs * R, 2 * BS), f32),
            pltpu.SemaphoreType.DMA((chunks + 1,)),
        ],
        mib=mib, flops=4 * n * R * ROWS * BS, nbytes=n * ROWS * BS * 2,
    )(col, f, g, own, slot, *f_edges, *fixed, weights)


def rhs_kernel(mid_ref, lo_ref, hi_ref, out_ref, up_ref, down_ref):
    out_ref[...] = mid_ref[...] + lo_ref[...].astype(f32) + hi_ref[...].astype(f32)
    up_ref[...] = out_ref[NB1 - EDGE :].astype(bf16)
    down_ref[...] = out_ref[:EDGE].astype(bf16)


def second_rhs(mid, lo, hi):
    return call(
        rhs_kernel, "rhs8",
        (shape((NB1, R, BS), f32), shape((EDGE, R, BS), bf16), shape((EDGE, R, BS), bf16)),
        [vmem()] * 3, (vmem(),) * 3, flops=2**18, nbytes=2**19,
    )(mid, lo, hi)


def spread(n, nc, e_ref, own_ref, slot_ref, device, x_ref, out_ref):
    highs = 3 * nc // 2

    def step(q, carry):
        t = pair_targets(own_ref, slot_ref, device, nc, q)
        rows = lax.broadcasted_iota(i32, (256, 256), 0)
        pick = jnp.where(rows == t % 256, 1.0, 0.0).astype(bf16)
        found = jnp.dot(e_ref[...], pick, preferred_element_type=f32)
        high = t // 256
        y = jnp.zeros((R, 256), f32)
        for h in range(highs):
            y = y + jnp.where(high == h, found[h * R : (h + 1) * R], 0.0)
        out_ref[2 * q] = x_ref[2 * q] + y[:, :BS]
        out_ref[2 * q + 1] = x_ref[2 * q + 1] + y[:, BS:]
        return carry

    lax.fori_loop(0, n // 2, step, 0)


def place(e_ref, b, value):
    e_ref[(b // 2) * R : (b // 2 + 1) * R, (b % 2) * BS : (b % 2 + 1) * BS] = value


def prolong_kernel(
    n, nc, own_ref, slot_ref, lo_ref, mid_ref, hi_ref, x_hbm, out_ref, first_ref, last_ref, e_ref, x_ref, sem
):
    copy = pltpu.make_async_copy(x_hbm, x_ref, sem.at[0])
    copy.start()
    for b in range(3 * nc):
        place(e_ref, b, (lo_ref, mid_ref, hi_ref)[b // nc][b % nc])
    copy.wait()
    spread(n, nc, e_ref, own_ref, slot_ref, device_index(), x_ref, out_ref)
    first_ref[...] = out_ref[:EDGE].astype(bf16)
    last_ref[...] = out_ref[n - EDGE :].astype(bf16)


def prolong(n, nc, own, slot, lo, mid, hi, x):
    return call(
        functools.partial(prolong_kernel, n, nc), f"prolong{n}",
        (shape((n, R, BS), f32), shape((EDGE, R, BS), bf16), shape((EDGE, R, BS), bf16)),
        [vmem()] * 5 + [hbm()],
        (vmem(),) * 3,
        [
            pltpu.VMEM((3 * nc // 2 * R, 2 * BS), bf16),
            pltpu.VMEM((n, R, BS), f32),
            pltpu.SemaphoreType.DMA((1,)),
        ],
        mib=12, flops=2 * n * BS * 3 * nc * BS * R, nbytes=2 * n * R * BS * 4,
    )(own, slot, lo, mid, hi, x)


def up_kernel(
    n, base, chunks,
    col_ref, x_ref, xlo_ref, xhi_ref, f_ref, g_ref, flo_ref, fhi_ref, slo_ref, shi_ref, w_hbm,
    *outs_and_scratch,
):
    *outs, w_ref, v0_ref, v1_ref, keep_ref, sem = outs_and_scratch
    out_ref = outs[0]
    copies = weight_copies(w_hbm, w_ref, sem, n, chunks)
    for c in copies:
        c.start()
    size = n // chunks
    start = device_index() * n

    def fill(b, carry):
        v0_ref[b + EDGE] = x_ref[b].astype(bf16)
        return carry

    lax.fori_loop(0, n, fill, 0, unroll=2)
    v0_ref[:EDGE] = xlo_ref[...]
    v0_ref[n + EDGE :] = xhi_ref[...]
    sides = []
    for side, fr, sr, xr in ((0, flo_ref, slo_ref, xlo_ref), (1, fhi_ref, shi_ref, xhi_ref)):
        near = read_near(sr[base + W_ROWS + 2 * EDGE : base + W_ROWS + 2 * EDGE + 1, :])
        sides.append((side, sr, xr, *edge_starts(base, fr, sr), near))
    for side, sr, xr, rhs, inv, near in sides:
        for i in range(HB):
            e = i + HB * (1 - side)
            j = i + side * (n + HB)
            w = sr[base + i * ROWS : base + (i + 1) * ROWS, :]
            p = product(v0_ref, [j + near[i * K + k] for k in range(K)], w)
            v1_ref[j] = (0.2 * xr[e].astype(f32) + inv[e] * (rhs(e) + p)).astype(bf16)

    def sweep(b, x, p):
        return 0.2 * x + (damping / g_ref[pl.ds(b, 1), :]) * (f_ref[b].astype(f32) + p)

    def near(b, base):
        return [b + base + near_of(col_ref, start, b, k) for k in range(K)]

    def first(b, carry):
        x = sweep(b, x_ref[b], product(v0_ref, near(b, HB), weight_of(w_ref, b)))
        keep_ref[b] = x
        v1_ref[b + HB] = x.astype(bf16)
        return carry

    for c in range(chunks):
        copies[c].wait()
        lax.fori_loop(c * size, (c + 1) * size, first, 0, unroll=4 if size % 4 == 0 else 2)

    def second(b, carry):
        p = product(v1_ref, near(b, 0), weight_of(w_ref, b))
        x = sweep(b, keep_ref[b], p).astype(out_ref.dtype)
        for ref in outs:
            ref[b] = x
        return carry

    lax.fori_loop(0, n, second, 0, unroll=4)


def go_up(n, base, col, x, x_edges, f, g, f_edges, fixed, weights, dtype, mib, outs=1):
    chunks = 4
    return call(
        functools.partial(up_kernel, n, base, chunks), f"up{n}",
        (shape((n, R, BS), dtype),) * outs,
        [smem()] + [vmem()] * 9 + [hbm()],
        (vmem(),) * outs,
        [
            pltpu.VMEM((n * ROWS, BS), bf16),
            pltpu.VMEM((n + 2 * EDGE, R, BS), bf16),
            pltpu.VMEM((n + EDGE, R, BS), bf16),
            pltpu.VMEM((n, R, BS), f32),
            pltpu.SemaphoreType.DMA((chunks,)),
        ],
        mib=mib, flops=4 * n * R * ROWS * BS, nbytes=n * ROWS * BS * 2,
    )(col, x, *x_edges, f, g, *f_edges, *fixed, weights)


def parts_kernel(low_ref, mid_ref, high_ref, out_ref, copy_ref):
    out_ref[:NB2] = low_ref[...]
    out_ref[NB2 : 2 * NB2] = mid_ref[...].astype(bf16)
    out_ref[2 * NB2 :] = high_ref[...]
    copy_ref[...] = out_ref[...]


def parts_of(low, mid, high):
    return call(
        parts_kernel, "parts", (shape((3 * NB2, R, BS), bf16),) * 2, [vmem()] * 3, (vmem(),) * 2,
        flops=2**17, nbytes=2**17,
    )(low, mid, high)


def window_kernel(mid_ref, p_ref, lo_ref, hi_ref, f_ref, up_ref, down_ref):
    a, b = NB2, 2 * NB2
    f_ref[...] = mid_ref[...] + lo_ref[b:].astype(f32) + hi_ref[:a].astype(f32)
    own = f_ref[...].astype(bf16)
    up_ref[:a] = own
    up_ref[a:b] = (hi_ref[a:b].astype(f32) + p_ref[b:].astype(f32)).astype(bf16)
    up_ref[b:] = hi_ref[b:]
    down_ref[:a] = own
    down_ref[a:b] = (lo_ref[a:b].astype(f32) + p_ref[:a].astype(f32)).astype(bf16)
    down_ref[b:] = lo_ref[:a]


def third_window(mid, p, lo, hi):
    return call(
        window_kernel, "window",
        (shape((NB2, R, BS), f32), shape((3 * NB2, R, BS), bf16), shape((3 * NB2, R, BS), bf16)),
        [vmem()] * 4, (vmem(),) * 3, flops=2**18, nbytes=2**18,
    )(mid, p, lo, hi)


REACH = 3


def third_fixed(w3_ref, tail_ref, slo_ref, shi_ref, rlo_ref, rhi_ref):
    at = NB2 * ROWS
    tails = {0: (tail_ref, 0), -1: (slo_ref, FIXED - TAIL), 1: (shi_ref, FIXED - TAIL)}
    tails[-3], tails[-2] = (rlo_ref, at), (rlo_ref, at + TAIL)
    tails[2], tails[3] = (rhi_ref, at + TAIL), (rhi_ref, at + 2 * TAIL)
    matrices = {0: (w3_ref, 0), -1: (slo_ref, EDGE2), 1: (shi_ref, EDGE2), -2: (rlo_ref, 0), 2: (rhi_ref, 0)}
    diagonal = []
    for d in range(-REACH, REACH + 1):
        ref, at = tails[d]
        diagonal += [diagonal_rows(ref, at, NB2, i) for i in range(NB2)]
    near = {}
    for d in range(-2, 3):
        ref, at = tails[d]
        near[d] = read_near(ref[at + 2 * NB2 : at + 2 * NB2 + 1, :])

    def weights(j):
        ref, at = matrices[j // NB2 - 2]
        return ref[at + (j % NB2) * ROWS : at + (j % NB2 + 1) * ROWS, :]

    def columns(j):
        return near[j // NB2 - 2][(j % NB2) * K : (j % NB2 + 1) * K]

    def row(d, kind):
        ref, at = tails[d]
        at = at + 2 * NB2 + 1 + kind * NB2
        return jnp.concatenate([ref[at + i : at + i + 1, :] for i in range(NB2)], axis=1).astype(f32).astype(i32)

    return diagonal, weights, columns, row


def third_down_kernel(
    f_ref, p_ref, lo_ref, hi_ref, dlo_ref, dhi_ref, w3_ref, tail_ref, slo_ref, shi_ref, rlo_ref, rhi_ref,
    c_ref, z_ref,
    v0_ref, v1_ref, v2_ref,
):
    diagonal, weights, columns, row = third_fixed(w3_ref, tail_ref, slo_ref, shi_ref, rlo_ref, rhi_ref)
    a, b = NB2, 2 * NB2
    wide = lambda ref, s, i: ref[s + i].astype(f32)
    f = []
    f += [wide(dlo_ref, 0, i) for i in range(a)]
    f += [wide(dlo_ref, a, i) + wide(lo_ref, 0, i) for i in range(a)]
    f += [wide(dlo_ref, b, i) + wide(lo_ref, a, i) + wide(p_ref, 0, i) for i in range(a)]
    f += [f_ref[i] for i in range(a)]
    f += [wide(dhi_ref, b, i) + wide(hi_ref, a, i) + wide(p_ref, b, i) for i in range(a)]
    f += [wide(dhi_ref, a, i) + wide(hi_ref, b, i) for i in range(a)]
    f += [wide(dhi_ref, 0, i) for i in range(a)]
    count = len(f)
    inv = [damping / g for g in diagonal]
    start = [f[i] * inv[i] for i in range(count)]
    for i in range(count):
        v0_ref[i] = start[i].astype(bf16)
    x1 = []
    for j in range(count - 4):
        p = product(v0_ref, [j + c for c in columns(j)], weights(j))
        x1.append(1.2 * start[j + 2] + inv[j + 2] * p)
        v1_ref[j] = x1[j].astype(bf16)
    res = []
    x2 = []
    for j in range(count - 8):
        p = product(v1_ref, [j + c for c in columns(j + 2)], weights(j + 2))
        r = f[j + 4] - diagonal[j + 4] * x1[j + 2] + p
        res.append(r)
        x2.append(x1[j + 2] + inv[j + 4] * r)
        v2_ref[j] = x2[j].astype(bf16)
    left = []
    right = []
    for d in (-1, 0, 1):
        r = jnp.concatenate(res[(d + 1) * a : (d + 2) * a], axis=1)
        left.append(jnp.where(row(d, 0) == -d, r, 0.0).astype(bf16))
        rows = lax.broadcasted_iota(i32, (C3, NB2 * BS), 0)
        right.append(jnp.where(rows == row(d, 1), 1.0, 0.0).astype(bf16))
    c = lax.dot_general(
        jnp.concatenate(left, axis=1), jnp.concatenate(right, axis=1),
        (((1,), (1,)), ((), ())), preferred_element_type=f32,
    ).astype(bf16)
    for i in range(c_ref.shape[0]):
        c_ref[i] = c
    for i in range(a):
        p = product(v2_ref, [i + c for c in columns(i + 4)], weights(i + 4))
        z_ref[i] = 0.2 * x2[i + 2] + start[i + 6] + inv[i + 6] * p


def third_down(copies, *args):
    count = 2 * NB2 * REACH + NB2
    return call(
        third_down_kernel, "down2",
        (shape((copies, R, C3), bf16), shape((NB2, R, BS), f32)),
        [vmem()] * 12, (vmem(),) * 2,
        [
            pltpu.VMEM((count, R, BS), bf16), pltpu.VMEM((count - 4, R, BS), bf16), pltpu.VMEM((count - 8, R, BS), bf16)
        ],
        mib=12, flops=2**27, nbytes=2**21,
    )(*args)


def coarse_kernel(got_ref, z_ref, s_hbm, out_ref, copy_ref, s_ref, sem):
    count = got_ref.shape[0]
    chunks = 4
    size = count // chunks
    copies = [
        pltpu.make_async_copy(s_hbm.at[:, pl.ds(c * size * BS, size * BS)], s_ref.at[c], sem.at[c])
        for c in range(chunks)
    ]
    for c in copies:
        c.start()
    u = jnp.zeros((R, C3), f32)
    for c in range(chunks):
        copies[c].wait()
        u = u + lax.dot_general(
            joined(got_ref, range(c * size, (c + 1) * size)), s_ref[c],
            (((1,), (1,)), ((), ())), preferred_element_type=f32,
        )
    out_ref[0] = u.astype(bf16)
    out_ref[1:] = z_ref[...].astype(bf16)
    copy_ref[...] = out_ref[...]


def coarse_solve(got, z, inverse_rows):
    count = got.shape[0]
    return call(
        coarse_kernel, "coarse", (shape((1 + NB2, R, BS), bf16),) * 2,
        [vmem(), vmem(), hbm()], (vmem(),) * 2,
        [pltpu.VMEM((4, C3, count // 4 * BS), bf16), pltpu.SemaphoreType.DMA((4,))],
        flops=2**26, nbytes=2**21,
    )(got, z, inverse_rows)


def three_kernel(lo_ref, own_ref, hi_ref, out_ref, copy_ref):
    out_ref[0] = lo_ref[0]
    out_ref[1] = own_ref[0]
    out_ref[2] = hi_ref[0]
    copy_ref[...] = out_ref[...]


def three_of(lo, own, hi):
    return call(
        three_kernel, "three", (shape((3, R, BS), bf16),) * 2, [vmem()] * 3, (vmem(),) * 2,
        flops=2**15, nbytes=2**16,
    )(lo, own, hi)


def third_up_kernel(
    own_ref, lo_ref, hi_ref, ulo_ref, uhi_ref, z_ref, w3_ref, tail_ref, slo_ref, shi_ref, rlo_ref, rhi_ref,
    own2_ref, slot2_ref, x_hbm,
    out_ref, first_ref, last_ref,
    v0_ref, v1_ref, e_ref, x_ref, sem,
):
    copy = pltpu.make_async_copy(x_hbm, x_ref, sem.at[0])
    copy.start()
    diagonal, weights, columns, row = third_fixed(w3_ref, tail_ref, slo_ref, shi_ref, rlo_ref, rhi_ref)
    inv = [damping / g for g in diagonal]
    u = [ulo_ref[0], ulo_ref[1], ulo_ref[2], lo_ref[0], own_ref[0], hi_ref[0], uhi_ref[0], uhi_ref[1], uhi_ref[2]]
    y = []
    for d in range(-REACH, REACH + 1):
        rows = lax.broadcasted_iota(i32, (C3, NB2 * BS), 0)
        pick = jnp.where(rows == row(d, 1), 1.0, 0.0).astype(bf16)
        at = d + REACH
        found = jnp.dot(jnp.concatenate(u[at : at + 3], axis=0), pick, preferred_element_type=f32)
        owner = row(d, 0)
        got = jnp.zeros((R, NB2 * BS), f32)
        for i in range(3):
            got = got + jnp.where(owner == i - 1, found[i * R : (i + 1) * R], 0.0)
        y += [got[:, i * BS : (i + 1) * BS] for i in range(NB2)]
    count = len(y)
    for i in range(count):
        v0_ref[i] = y[i].astype(bf16)
    y1 = []
    for j in range(count - 4):
        p = product(v0_ref, [j + c for c in columns(j)], weights(j))
        y1.append(0.2 * y[j + 2] + inv[j + 2] * p)
        v1_ref[j] = y1[j].astype(bf16)
    for j in range(count - 8):
        p = product(v1_ref, [j + c for c in columns(j + 2)], weights(j + 2))
        y2 = 0.2 * y1[j + 2] + inv[j + 4] * p
        i = j % NB2
        z = (lambda: lo_ref[1 + i].astype(f32), lambda: z_ref[i], lambda: hi_ref[1 + i].astype(f32))[j // NB2]()
        place(e_ref, j, (z + y2).astype(bf16))
    copy.wait()
    spread(NB1, NB2, e_ref, own2_ref, slot2_ref, device_index(), x_ref, out_ref)
    first_ref[...] = out_ref[:EDGE].astype(bf16)
    last_ref[...] = out_ref[NB1 - EDGE :].astype(bf16)


def third_up(*args):
    count = 2 * NB2 * REACH + NB2
    return call(
        third_up_kernel, "up2",
        (shape((NB1, R, BS), f32), shape((EDGE, R, BS), bf16), shape((EDGE, R, BS), bf16)),
        [vmem()] * 14 + [hbm()], (vmem(),) * 3,
        [
            pltpu.VMEM((count, R, BS), bf16), pltpu.VMEM((count - 4, R, BS), bf16),
            pltpu.VMEM((3 * NB2 // 2 * R, 2 * BS), bf16), pltpu.VMEM((NB1, R, BS), f32),
            pltpu.SemaphoreType.DMA((1,)),
        ],
        mib=12, flops=2**27, nbytes=2**21,
    )(*args)


def on_device(
    right_sides,
    weights_fine, columns_fine, degree_fine, owners_fine, slots_fine,
    weights_second, columns_second, degree_second, owners_second, slots_second,
    weights_third, columns_third, degree_third, owners_third, slots_third,
    coarse_inverse,
):
    flat = lambda a: a.reshape(-1, BS)
    f = right_sides
    columns_fine, columns_second, columns_third = columns_fine.T, columns_second.T, columns_third.T
    w1, w2, w3 = (in_hbm(flat(w)) for w in (weights_fine, weights_second, weights_third))
    coarse_inverse = in_hbm(coarse_inverse)
    edges1 = both_ways(*first_edges(in_hbm(flat(f)), w1, degree_fine, columns_fine))
    g1, g2, _, up, down, w3, tail = fixed_data(
        w1, w2, w3, degree_fine, degree_second, degree_third, columns_second, columns_third, owners_third, slots_third
    )
    fixed = both_ways(up, down)
    far = both_ways(*far_data(w3, tail, *fixed), 2)
    third = (w3, tail, *fixed, *far)

    x1, low, mid, high = go_down(
        NB0, NB1, F_ROWS, columns_fine, f, g1, owners_fine, slots_fine, edges1, edges1, w1, 20
    )
    lo, hi = both_ways(high, low)
    f2, up, down = second_rhs(mid, lo, hi)
    f_edges = both_ways(up, down)
    x2, low, mid, high = go_down(
        NB1, NB2, 0, columns_second, f2, g2, owners_second, slots_second, f_edges, fixed, w2, 12
    )
    parts, copy = parts_of(low, mid, high)
    plo, phi = both_ways(copy, parts)
    f3, up, down = third_window(mid, parts, plo, phi)
    dlo, dhi = both_ways(up, down, 3)
    c, z = third_down(lax.axis_size("col"), f3, parts, plo, phi, dlo, dhi, *third)
    got = lax.all_to_all(c, "col", 0, 0, tiled=True)
    own, copy = coarse_solve(got, z, coarse_inverse)
    lo, hi = both_ways(copy, own)
    near, copy = three_of(lo, own, hi)
    ulo, uhi = both_ways(near, copy, 3)
    x2, first, last = third_up(own, lo, hi, ulo, uhi, z, *third, owners_second, slots_second, x2)
    x_edges = both_ways(last, first)
    x2, copy = go_up(NB1, 0, columns_second, x2, x_edges, f2, g2, f_edges, fixed, w2, bf16, 12, 2)
    lo, hi = both_ways(copy, x2)
    x1, first, last = prolong(NB0, NB1, owners_fine, slots_fine, lo, x2, hi, x1)
    x_edges = both_ways(last, first)
    return go_up(NB0, F_ROWS, columns_fine, x1, x_edges, f, g1, edges1, edges1, w1, f32, 20)[0]


def solution(mesh):
    block = P(AXES, None, None)
    pair = P(AXES, None)
    four = P(AXES, None, None, None)
    level = (four, pair, pair, pair, pair)
    return jax.shard_map(
        on_device, mesh=mesh, in_specs=(block, *level, *level, *level, pair), out_specs=block, check_vma=False
    )
```

```python
import functools

import jax
import jax.numpy as jnp
from jax import lax
from jax.experimental import pallas as pl
from jax.experimental.pallas import tpu as pltpu
from jax.sharding import PartitionSpec as P

BS = 128
R = 64
K = 3
HB = 2
NB2 = 2
NB1 = 8
NB0 = 32
C3 = 128
AXES = ("row", "col")
EDGE = 2 * HB
ROWS = K * BS
damping = 0.8
bf16 = jnp.bfloat16
f32 = jnp.float32
i32 = jnp.int32
INV = 1.0 / (K * BS)

F_ROWS = EDGE * R
W_ROWS = HB * ROWS
TAIL = 16
EDGE1 = F_ROWS + W_ROWS + TAIL
EDGE2 = W_ROWS + TAIL
THIRD = NB2 * ROWS + TAIL
FIXED = EDGE2 + THIRD
FAR = NB2 * ROWS + 3 * TAIL


def passed_along(value, steps):
    count = lax.axis_size(AXES)
    return lax.ppermute(value, AXES, [(s, (s + steps) % count) for s in range(count)])


def both_ways(up, down, steps=1):
    return passed_along(up, steps), passed_along(down, -steps)


def in_hbm(x):
    return pltpu.with_memory_space_constraint(x, pltpu.HBM)


def vmem():
    return pl.BlockSpec(memory_space=pltpu.VMEM)


def smem():
    return pl.BlockSpec(memory_space=pltpu.SMEM)


def hbm():
    return pl.BlockSpec(memory_space=pltpu.HBM)


def shape(dims, dtype):
    return jax.ShapeDtypeStruct(dims, dtype)


def call(kernel, name, outs, in_specs, out_specs, scratch=(), mib=6, flops=0, nbytes=0):
    return pl.pallas_call(
        kernel,
        out_shape=outs,
        in_specs=in_specs,
        out_specs=out_specs,
        scratch_shapes=list(scratch),
        compiler_params=pltpu.CompilerParams(vmem_limit_bytes=mib * 1024 * 1024),
        cost_estimate=pl.CostEstimate(flops=flops, transcendentals=0, bytes_accessed=nbytes),
        name=name,
    )


def device_index():
    return lax.axis_index(AXES)


def near_row(values):
    lane = lax.broadcasted_iota(i32, (1, BS), 1)
    row = jnp.zeros((1, BS), f32)
    for i, v in enumerate(values):
        row = jnp.where(lane == i, v.astype(f32), row)
    return row


def read_near(row):
    lane = lax.broadcasted_iota(i32, (1, BS), 1)
    row = row.astype(f32)
    return [jnp.sum(jnp.where(lane == i, row, 0.0)).astype(i32) for i in range(HB * K)]


def near_of(col_ref, first, b, k):
    return col_ref[k, b] - (first + b - HB)


def column_sum(w):
    return jnp.sum(w.astype(f32), axis=0, keepdims=True)


def diagonal_rows(ref, at, stride, i):
    return ref[at + i : at + i + 1, :].astype(f32) + ref[at + stride + i : at + stride + i + 1, :].astype(f32)


def inverse(g):
    return jnp.where(g > 0, damping / g, 0.0)


def joined(v_ref, indices):
    return jnp.concatenate([v_ref[i] for i in indices], axis=1)


def product(v_ref, indices, w):
    return jnp.dot(joined(v_ref, indices), w, preferred_element_type=f32) * INV


def tail_rows(gs, nears, extra=()):
    high = [g.astype(bf16).astype(f32) for g in gs]
    low = [g - h for g, h in zip(gs, high)]
    rows = high + low + [near_row(nears)] + list(extra)
    rows = rows + [jnp.zeros((1, BS), f32)] * (TAIL - len(rows))
    return jnp.concatenate(rows, axis=0).astype(bf16)


def edge_kernel(f_hbm, w_hbm, deg_hbm, col_hbm, up_ref, down_ref, w_ref, deg_ref, col_ref, sem):
    n = NB0
    small = [
        pltpu.make_async_copy(deg_hbm, deg_ref, sem.at[6]),
        pltpu.make_async_copy(col_hbm, col_ref, sem.at[7]),
    ]
    first = device_index() * n
    copies = [
        pltpu.make_async_copy(w_hbm.at[pl.ds((n - EDGE) * ROWS, EDGE * ROWS)], w_ref.at[1], sem.at[0]),
        pltpu.make_async_copy(w_hbm.at[pl.ds(0, EDGE * ROWS)], w_ref.at[0], sem.at[1]),
        pltpu.make_async_copy(f_hbm.at[pl.ds((n - EDGE) * R, F_ROWS)], up_ref.at[pl.ds(0, F_ROWS)], sem.at[2]),
        pltpu.make_async_copy(f_hbm.at[pl.ds(0, F_ROWS)], down_ref.at[pl.ds(0, F_ROWS)], sem.at[3]),
        pltpu.make_async_copy(
            w_hbm.at[pl.ds((n - HB) * ROWS, W_ROWS)], up_ref.at[pl.ds(F_ROWS, W_ROWS)], sem.at[4]
        ),
        pltpu.make_async_copy(w_hbm.at[pl.ds(0, W_ROWS)], down_ref.at[pl.ds(F_ROWS, W_ROWS)], sem.at[5]),
    ]
    for c in small + copies:
        c.start()
    for c in small:
        c.wait()
    for side, ref, start, near_start in ((1, up_ref, n - EDGE, n - HB), (0, down_ref, 0, 0)):
        copies[1 - side].wait()
        gs = [
            deg_ref[start + i : start + i + 1, :] + column_sum(w_ref[side, i * ROWS : (i + 1) * ROWS, :]) * INV
            for i in range(EDGE)
        ]
        nears = [near_of(col_ref, first, near_start + i, k) for i in range(HB) for k in range(K)]
        ref[F_ROWS + W_ROWS :, :] = tail_rows(gs, nears)
    for c in copies[2:]:
        c.wait()


def first_edges(f, w, deg, col):
    return call(
        edge_kernel, "edges",
        (shape((EDGE1, BS), bf16),) * 2,
        [hbm()] * 4,
        (vmem(),) * 2,
        [
            pltpu.VMEM((2, EDGE * ROWS, BS), bf16),
            pltpu.VMEM((NB0, BS), f32),
            pltpu.SMEM((K, NB0), i32),
            pltpu.SemaphoreType.DMA((8,)),
        ],
        flops=2**20, nbytes=2**21,
    )(f, w, deg, col)


def fixed_kernel(
    w1_hbm, w2_hbm, w3_hbm, deg1_ref, deg2_ref, deg3_ref, col2_ref, col3_ref, own3_ref, slot3_ref,
    g1_ref, g2_ref, g3_ref, up_ref, down_ref, w3_ref, tail_ref, w1_ref, w2_ref, sem,
):
    device = device_index()
    chunks = 4
    size = NB0 // chunks
    last3 = pltpu.make_async_copy(w3_hbm, w3_ref, sem.at[0])
    last2 = pltpu.make_async_copy(w2_hbm, w2_ref, sem.at[1])
    copies = [
        pltpu.make_async_copy(
            w2_hbm.at[pl.ds((NB1 - HB) * ROWS, W_ROWS)], up_ref.at[pl.ds(0, W_ROWS)], sem.at[2]
        ),
        pltpu.make_async_copy(w2_hbm.at[pl.ds(0, W_ROWS)], down_ref.at[pl.ds(0, W_ROWS)], sem.at[3]),
        pltpu.make_async_copy(w3_hbm, up_ref.at[pl.ds(EDGE2, W_ROWS)], sem.at[4]),
        pltpu.make_async_copy(w3_hbm, down_ref.at[pl.ds(EDGE2, W_ROWS)], sem.at[5]),
    ]
    bulk = [
        pltpu.make_async_copy(
            w1_hbm.at[pl.ds(c * size * ROWS, size * ROWS)], w1_ref.at[pl.ds(c * size * ROWS, size * ROWS)], sem.at[6 + c]
        )
        for c in range(chunks)
    ]
    for c in [last3, last2] + copies + bulk:
        c.start()
    last3.wait()
    g3 = [deg3_ref[i : i + 1, :] + column_sum(w3_ref[i * ROWS : (i + 1) * ROWS, :]) * INV for i in range(NB2)]
    for i in range(NB2):
        g3_ref[i : i + 1, :] = g3[i]
    nears = [near_of(col3_ref, device * NB2, i, k) for i in range(NB2) for k in range(K)]
    extra = [(own3_ref[i : i + 1, :] - device).astype(f32) for i in range(NB2)]
    extra = extra + [slot3_ref[i : i + 1, :].astype(f32) for i in range(NB2)]
    tail = tail_rows(g3, nears, extra)
    tail_ref[...] = tail
    up_ref[EDGE2 + W_ROWS :, :] = tail
    down_ref[EDGE2 + W_ROWS :, :] = tail
    last2.wait()
    g2 = [deg2_ref[i : i + 1, :] + column_sum(w2_ref[i * ROWS : (i + 1) * ROWS, :]) * INV for i in range(NB1)]
    for i in range(NB1):
        g2_ref[i : i + 1, :] = g2[i]
    first = device * NB1
    up_ref[W_ROWS : W_ROWS + TAIL, :] = tail_rows(
        g2[NB1 - EDGE :], [near_of(col2_ref, first, NB1 - HB + i, k) for i in range(HB) for k in range(K)]
    )
    down_ref[W_ROWS : W_ROWS + TAIL, :] = tail_rows(
        g2[:EDGE], [near_of(col2_ref, first, i, k) for i in range(HB) for k in range(K)]
    )

    def one(b, carry):
        at = pl.multiple_of(b * ROWS, ROWS)
        g1_ref[pl.ds(b, 1), :] = deg1_ref[pl.ds(b, 1), :] + column_sum(w1_ref[pl.ds(at, ROWS), :]) * INV
        return carry

    for c in range(chunks):
        bulk[c].wait()
        lax.fori_loop(c * size, (c + 1) * size, one, 0, unroll=2)
    for c in copies:
        c.wait()


def fixed_data(w1, w2, w3, deg1, deg2, deg3, col2, col3, own3, slot3):
    return call(
        fixed_kernel, "fixed",
        (
            shape((NB0, BS), f32), shape((NB1, BS), f32), shape((NB2, BS), f32),
            shape((FIXED, BS), bf16), shape((FIXED, BS), bf16),
            shape((NB2 * ROWS, BS), bf16), shape((TAIL, BS), bf16), shape((NB0 * ROWS, BS), bf16),
        ),
        [hbm()] * 3 + [vmem()] * 3 + [smem()] * 2 + [vmem()] * 2,
        (vmem(),) * 8,
        [
            pltpu.VMEM((NB1 * ROWS, BS), bf16),
            pltpu.SemaphoreType.DMA((10,)),
        ],
        mib=10, flops=2**30, nbytes=2**22,
    )(w1, w2, w3, deg1, deg2, deg3, col2, col3, own3, slot3)


def far_kernel(w3_ref, tail_ref, lo_ref, hi_ref, out_ref, copy_ref):
    at = NB2 * ROWS
    out_ref[:at, :] = w3_ref[...]
    out_ref[at : at + TAIL, :] = lo_ref[FIXED - TAIL :, :]
    out_ref[at + TAIL : at + 2 * TAIL, :] = tail_ref[...]
    out_ref[at + 2 * TAIL :, :] = hi_ref[FIXED - TAIL :, :]
    copy_ref[...] = out_ref[...]


def far_data(w3, tail, lo, hi):
    return call(
        far_kernel, "far", (shape((FAR, BS), bf16),) * 2, [vmem()] * 4, (vmem(),) * 2, flops=2**20, nbytes=2**19
    )(w3, tail, lo, hi)


def weight_copies(w_hbm, w_ref, sem, n, chunks):
    size = n // chunks * ROWS
    return [
        pltpu.make_async_copy(w_hbm.at[pl.ds(c * size, size)], w_ref.at[pl.ds(c * size, size)], sem.at[c])
        for c in range(chunks)
    ]


def weight_of(w_ref, b):
    return w_ref[pl.ds(pl.multiple_of(b * ROWS, ROWS), ROWS), :]


def edge_starts(base, f_ref, s_ref):
    if base:
        rhs = lambda i: f_ref[i * R : (i + 1) * R, :].astype(f32)
    else:
        rhs = lambda i: f_ref[i].astype(f32)
    inv = [inverse(diagonal_rows(s_ref, base + W_ROWS, EDGE, i)) for i in range(EDGE)]
    return rhs, inv


def down_kernel(
    n, nc, base, chunks,
    col_ref, f_ref, g_ref, own_ref, slot_ref, flo_ref, fhi_ref, slo_ref, shi_ref, *rest,
):
    inner_ref = None
    if chunks:
        w_hbm, x_ref, down_ref, mid_ref, up_ref, v0_ref, v1_ref, r_ref, acc_ref, w_ref, sem = rest
        copies = weight_copies(w_hbm, w_ref, sem, n, chunks)
        for c in copies:
            c.start()
        size = n // chunks
    else:
        w_ref, inner_ref, x_ref, down_ref, mid_ref, up_ref, v0_ref, v1_ref, r_ref, acc_ref = rest
    device = device_index()
    start = device * n

    def scale(b):
        return damping / g_ref[pl.ds(b, 1), :]

    def fill(b, carry):
        v0_ref[b + EDGE] = (f_ref[b].astype(f32) * scale(b)).astype(bf16)
        return carry

    lax.fori_loop(0, n, fill, 0, unroll=2)
    sides = []
    for side, fr, sr in ((0, flo_ref, slo_ref), (1, fhi_ref, shi_ref)):
        rhs, inv = edge_starts(base, fr, sr)
        starts = [rhs(i) * inv[i] for i in range(EDGE)]
        for i in range(EDGE):
            v0_ref[i + side * (n + EDGE)] = starts[i].astype(bf16)
        near = read_near(sr[base + W_ROWS + 2 * EDGE : base + W_ROWS + 2 * EDGE + 1, :])
        sides.append((side, sr, starts, inv, near))
    for side, sr, starts, inv, near in sides:
        for i in range(HB):
            e = i + HB * (1 - side)
            j = i + side * (n + HB)
            w = sr[base + i * ROWS : base + (i + 1) * ROWS, :]
            p = product(v0_ref, [j + near[i * K + k] for k in range(K)], w)
            v1_ref[j] = (1.2 * starts[e] + inv[e] * p).astype(bf16)

    def first(b, carry):
        p = product(v0_ref, [b + HB + near_of(col_ref, start, b, k) for k in range(K)], weight_of(w_ref, b))
        s = scale(b)
        x = 1.2 * (f_ref[b].astype(f32) * s) + s * p
        x_ref[b] = x
        v1_ref[b + HB] = x.astype(bf16)
        return carry

    for c in range(chunks):
        copies[c].wait()
        lax.fori_loop(c * size, (c + 1) * size, first, 0, unroll=4 if size % 4 == 0 else 2)
    if not chunks:
        take_inner(n, inner_ref, x_ref, v1_ref)
        for b in edge_blocks(n):
            first(b, 0)

    def residual(b):
        p = product(v1_ref, [b + near_of(col_ref, start, b, k) for k in range(K)], weight_of(w_ref, b))
        return f_ref[b].astype(f32) - g_ref[pl.ds(b, 1), :] * x_ref[b] + p

    def second(q, carry):
        r_ref[q] = jnp.concatenate([residual(2 * q), residual(2 * q + 1)], axis=1).astype(bf16)
        return carry

    lax.fori_loop(0, n // 2, second, 0, unroll=2)

    highs = 3 * nc // 2
    group = 4
    acc_ref[...] = jnp.zeros_like(acc_ref)

    def gather(q, carry):
        left = []
        right = []
        for i in range(group):
            t = pair_targets(own_ref, slot_ref, device, nc, q * group + i)
            r = r_ref[q * group + i]
            high = t // 256
            left.append(
                jnp.concatenate([r * jnp.where(high == h, 1.0, 0.0).astype(bf16) for h in range(highs)], axis=0)
            )
            rows = lax.broadcasted_iota(i32, (256, 256), 0)
            right.append(jnp.where(rows == t % 256, 1.0, 0.0).astype(bf16))
        acc_ref[...] += lax.dot_general(
            jnp.concatenate(left, axis=1),
            jnp.concatenate(right, axis=1),
            (((1,), (1,)), ((), ())),
            preferred_element_type=f32,
        )
        return carry

    lax.fori_loop(0, n // 2 // group, gather, 0)

    for b in range(3 * nc):
        part = acc_ref[(b // 2) * R : (b // 2 + 1) * R, (b % 2) * BS : (b % 2 + 1) * BS]
        where = b // nc
        ref = (down_ref, mid_ref, up_ref)[where]
        ref[b - where * nc] = part.astype(ref.dtype)


def edge_blocks(n):
    return list(range(HB)) + list(range(n - HB, n))


def take_inner(n, inner_ref, x_ref, v_ref):
    def one(b, carry):
        x = inner_ref[b]
        x_ref[b] = x
        v_ref[b + HB] = x.astype(bf16)
        return carry

    lax.fori_loop(HB, n - HB, one, 0, unroll=4)


def pair_targets(own_ref, slot_ref, device, nc, q):
    row = lambda b: (own_ref[pl.ds(b, 1), :] - device + 1) * (nc * BS) + slot_ref[pl.ds(b, 1), :]
    return jnp.concatenate([row(2 * q), row(2 * q + 1)], axis=1)


def go_down(n, nc, base, col, f, g, own, slot, f_edges, fixed, weights, mib, inner=None):
    chunks = 0 if inner is not None else 4
    loads = [pltpu.VMEM((n * ROWS, BS), bf16), pltpu.SemaphoreType.DMA((4,))] if chunks else []
    last = (weights,) if chunks else (weights, inner)
    highs = 3 * nc // 2
    return call(
        functools.partial(down_kernel, n, nc, base, chunks), f"down{n}",
        (
            shape((n, R, BS), f32), shape((nc, R, BS), bf16), shape((nc, R, BS), f32), shape((nc, R, BS), bf16)
        ),
        [smem()] + [vmem()] * 8 + ([hbm()] if chunks else [vmem()] * 2),
        (vmem(),) * 4,
        [
            pltpu.VMEM((n + 2 * EDGE, R, BS), bf16),
            pltpu.VMEM((n + EDGE, R, BS), bf16),
            pltpu.VMEM((n // 2, R, 2 * BS), bf16),
            pltpu.VMEM((highs * R, 2 * BS), f32),
            *loads,
        ],
        mib=mib, flops=4 * n * R * ROWS * BS, nbytes=n * ROWS * BS * 2,
    )(col, f, g, own, slot, *f_edges, *fixed, *last)


def rhs_kernel(mid_ref, lo_ref, hi_ref, out_ref, up_ref, down_ref):
    out_ref[...] = mid_ref[...] + lo_ref[...].astype(f32) + hi_ref[...].astype(f32)
    up_ref[...] = out_ref[NB1 - EDGE :].astype(bf16)
    down_ref[...] = out_ref[:EDGE].astype(bf16)


def second_rhs(mid, lo, hi):
    return call(
        rhs_kernel, "rhs8",
        (shape((NB1, R, BS), f32), shape((EDGE, R, BS), bf16), shape((EDGE, R, BS), bf16)),
        [vmem()] * 3, (vmem(),) * 3, flops=2**18, nbytes=2**19,
    )(mid, lo, hi)


def spread(n, nc, e_ref, own_ref, slot_ref, device, x_ref, out_ref):
    highs = 3 * nc // 2

    def step(q, carry):
        t = pair_targets(own_ref, slot_ref, device, nc, q)
        rows = lax.broadcasted_iota(i32, (256, 256), 0)
        pick = jnp.where(rows == t % 256, 1.0, 0.0).astype(bf16)
        found = jnp.dot(e_ref[...], pick, preferred_element_type=f32)
        high = t // 256
        y = jnp.zeros((R, 256), f32)
        for h in range(highs):
            y = y + jnp.where(high == h, found[h * R : (h + 1) * R], 0.0)
        out_ref[2 * q] = x_ref[2 * q] + y[:, :BS]
        out_ref[2 * q + 1] = x_ref[2 * q + 1] + y[:, BS:]
        return carry

    lax.fori_loop(0, n // 2, step, 0)


def place(e_ref, b, value):
    e_ref[(b // 2) * R : (b // 2 + 1) * R, (b % 2) * BS : (b % 2 + 1) * BS] = value


def prolong_kernel(
    n, nc, own_ref, slot_ref, lo_ref, mid_ref, hi_ref, x_ref, out_ref, first_ref, last_ref, e_ref
):
    for b in range(3 * nc):
        place(e_ref, b, (lo_ref, mid_ref, hi_ref)[b // nc][b % nc])
    spread(n, nc, e_ref, own_ref, slot_ref, device_index(), x_ref, out_ref)
    first_ref[...] = out_ref[:EDGE].astype(bf16)
    last_ref[...] = out_ref[n - EDGE :].astype(bf16)


def prolong(n, nc, own, slot, lo, mid, hi, x):
    return call(
        functools.partial(prolong_kernel, n, nc), f"prolong{n}",
        (shape((n, R, BS), f32), shape((EDGE, R, BS), bf16), shape((EDGE, R, BS), bf16)),
        [vmem()] * 6,
        (vmem(),) * 3,
        [pltpu.VMEM((3 * nc // 2 * R, 2 * BS), bf16)],
        mib=12, flops=2 * n * BS * 3 * nc * BS * R, nbytes=2 * n * R * BS * 4,
    )(own, slot, lo, mid, hi, x)


def up_kernel(
    n, base, chunks,
    col_ref, x_ref, xlo_ref, xhi_ref, f_ref, g_ref, flo_ref, fhi_ref, slo_ref, shi_ref, w_ref, *rest,
):
    inner_ref = None
    if chunks:
        *outs, v0_ref, v1_ref, keep_ref, kept_ref, sem = rest
        copies = weight_copies(w_ref, kept_ref, sem, n, chunks)
        w_ref = kept_ref
        for c in copies:
            c.start()
        size = n // chunks
    else:
        inner_ref, *outs, v0_ref, v1_ref, keep_ref = rest
    out_ref = outs[0]
    start = device_index() * n

    def fill(b, carry):
        v0_ref[b + EDGE] = x_ref[b].astype(bf16)
        return carry

    lax.fori_loop(0, n, fill, 0, unroll=2)
    v0_ref[:EDGE] = xlo_ref[...]
    v0_ref[n + EDGE :] = xhi_ref[...]
    sides = []
    for side, fr, sr, xr in ((0, flo_ref, slo_ref, xlo_ref), (1, fhi_ref, shi_ref, xhi_ref)):
        near = read_near(sr[base + W_ROWS + 2 * EDGE : base + W_ROWS + 2 * EDGE + 1, :])
        sides.append((side, sr, xr, *edge_starts(base, fr, sr), near))
    for side, sr, xr, rhs, inv, near in sides:
        for i in range(HB):
            e = i + HB * (1 - side)
            j = i + side * (n + HB)
            w = sr[base + i * ROWS : base + (i + 1) * ROWS, :]
            p = product(v0_ref, [j + near[i * K + k] for k in range(K)], w)
            v1_ref[j] = (0.2 * xr[e].astype(f32) + inv[e] * (rhs(e) + p)).astype(bf16)

    def sweep(b, x, p):
        return 0.2 * x + (damping / g_ref[pl.ds(b, 1), :]) * (f_ref[b].astype(f32) + p)

    def near(b, base):
        return [b + base + near_of(col_ref, start, b, k) for k in range(K)]

    def first(b, carry):
        x = sweep(b, x_ref[b], product(v0_ref, near(b, HB), weight_of(w_ref, b)))
        keep_ref[b] = x
        v1_ref[b + HB] = x.astype(bf16)
        return carry

    for c in range(chunks):
        copies[c].wait()
        lax.fori_loop(c * size, (c + 1) * size, first, 0, unroll=4 if size % 4 == 0 else 2)
    if not chunks:
        take_inner(n, inner_ref, keep_ref, v1_ref)
        for b in edge_blocks(n):
            first(b, 0)

    def second(b, carry):
        p = product(v1_ref, near(b, 0), weight_of(w_ref, b))
        x = sweep(b, keep_ref[b], p).astype(out_ref.dtype)
        for ref in outs:
            ref[b] = x
        return carry

    lax.fori_loop(0, n, second, 0, unroll=4)


def go_up(n, base, col, x, x_edges, f, g, f_edges, fixed, weights, dtype, mib, outs=1, inner=None):
    chunks = 0 if inner is not None else 4
    loads = [pltpu.VMEM((n * ROWS, BS), bf16), pltpu.SemaphoreType.DMA((4,))] if chunks else []
    last = (weights,) if chunks else (weights, inner)
    return call(
        functools.partial(up_kernel, n, base, chunks), f"up{n}",
        (shape((n, R, BS), dtype),) * outs,
        [smem()] + [vmem()] * 9 + ([hbm()] if chunks else [vmem()] * 2),
        (vmem(),) * outs,
        [
            pltpu.VMEM((n + 2 * EDGE, R, BS), bf16),
            pltpu.VMEM((n + EDGE, R, BS), bf16),
            pltpu.VMEM((n, R, BS), f32),
            *loads,
        ],
        mib=mib, flops=4 * n * R * ROWS * BS, nbytes=n * ROWS * BS * 2,
    )(col, x, *x_edges, f, g, *f_edges, *fixed, *last)


def inner_kernel(n, first_sweep, col_ref, x_ref, f_ref, g_ref, w_ref, out_ref, v_ref):
    start = device_index() * n

    def scale(b):
        return damping / g_ref[pl.ds(b, 1), :]

    def fill(b, carry):
        x = f_ref[b].astype(f32) * scale(b) if first_sweep else x_ref[b]
        v_ref[b] = x.astype(bf16)
        return carry

    lax.fori_loop(0, n, fill, 0, unroll=4)

    def one(b, carry):
        p = product(v_ref, [b - HB + near_of(col_ref, start, b, k) for k in range(K)], weight_of(w_ref, b))
        s = scale(b)
        f = f_ref[b].astype(f32)
        out_ref[b] = 1.2 * (f * s) + s * p if first_sweep else 0.2 * x_ref[b] + s * (f + p)
        return carry

    lax.fori_loop(HB, n - HB, one, 0, unroll=4)
    blank = jnp.zeros((R, BS), f32)
    for b in list(range(HB)) + list(range(n - HB, n)):
        out_ref[b] = blank


def inner_sweep(n, first_sweep, col, x, f, g, w):
    return call(
        functools.partial(inner_kernel, n, first_sweep), "inner" + ("down" if first_sweep else "up"),
        shape((n, R, BS), f32),
        [smem()] + [vmem()] * 4, vmem(), [pltpu.VMEM((n, R, BS), bf16)],
        mib=12, flops=2 * n * R * ROWS * BS, nbytes=2**20,
    )(col, x, f, g, w)


def parts_kernel(low_ref, mid_ref, high_ref, out_ref, copy_ref):
    out_ref[:NB2] = low_ref[...]
    out_ref[NB2 : 2 * NB2] = mid_ref[...].astype(bf16)
    out_ref[2 * NB2 :] = high_ref[...]
    copy_ref[...] = out_ref[...]


def parts_of(low, mid, high):
    return call(
        parts_kernel, "parts", (shape((3 * NB2, R, BS), bf16),) * 2, [vmem()] * 3, (vmem(),) * 2,
        flops=2**17, nbytes=2**17,
    )(low, mid, high)


def window_kernel(mid_ref, p_ref, lo_ref, hi_ref, f_ref, up_ref, down_ref):
    a, b = NB2, 2 * NB2
    f_ref[...] = mid_ref[...] + lo_ref[b:].astype(f32) + hi_ref[:a].astype(f32)
    own = f_ref[...].astype(bf16)
    up_ref[:a] = own
    up_ref[a:b] = (hi_ref[a:b].astype(f32) + p_ref[b:].astype(f32)).astype(bf16)
    up_ref[b:] = hi_ref[b:]
    down_ref[:a] = own
    down_ref[a:b] = (lo_ref[a:b].astype(f32) + p_ref[:a].astype(f32)).astype(bf16)
    down_ref[b:] = lo_ref[:a]


def third_window(mid, p, lo, hi):
    return call(
        window_kernel, "window",
        (shape((NB2, R, BS), f32), shape((3 * NB2, R, BS), bf16), shape((3 * NB2, R, BS), bf16)),
        [vmem()] * 4, (vmem(),) * 3, flops=2**18, nbytes=2**18,
    )(mid, p, lo, hi)


REACH = 3


def third_fixed(w3_ref, tail_ref, slo_ref, shi_ref, rlo_ref, rhi_ref):
    at = NB2 * ROWS
    tails = {0: (tail_ref, 0), -1: (slo_ref, FIXED - TAIL), 1: (shi_ref, FIXED - TAIL)}
    tails[-3], tails[-2] = (rlo_ref, at), (rlo_ref, at + TAIL)
    tails[2], tails[3] = (rhi_ref, at + TAIL), (rhi_ref, at + 2 * TAIL)
    matrices = {0: (w3_ref, 0), -1: (slo_ref, EDGE2), 1: (shi_ref, EDGE2), -2: (rlo_ref, 0), 2: (rhi_ref, 0)}
    diagonal = []
    for d in range(-REACH, REACH + 1):
        ref, at = tails[d]
        diagonal += [diagonal_rows(ref, at, NB2, i) for i in range(NB2)]
    near = {}
    for d in range(-2, 3):
        ref, at = tails[d]
        near[d] = read_near(ref[at + 2 * NB2 : at + 2 * NB2 + 1, :])

    def weights(j):
        ref, at = matrices[j // NB2 - 2]
        return ref[at + (j % NB2) * ROWS : at + (j % NB2 + 1) * ROWS, :]

    def columns(j):
        return near[j // NB2 - 2][(j % NB2) * K : (j % NB2 + 1) * K]

    def row(d, kind):
        ref, at = tails[d]
        at = at + 2 * NB2 + 1 + kind * NB2
        return jnp.concatenate([ref[at + i : at + i + 1, :] for i in range(NB2)], axis=1).astype(f32).astype(i32)

    return diagonal, weights, columns, row


def third_down_kernel(
    f_ref, p_ref, lo_ref, hi_ref, dlo_ref, dhi_ref, w3_ref, tail_ref, slo_ref, shi_ref, rlo_ref, rhi_ref,
    c_ref, z_ref,
    v0_ref, v1_ref, v2_ref,
):
    diagonal, weights, columns, row = third_fixed(w3_ref, tail_ref, slo_ref, shi_ref, rlo_ref, rhi_ref)
    a, b = NB2, 2 * NB2
    wide = lambda ref, s, i: ref[s + i].astype(f32)
    f = []
    f += [wide(dlo_ref, 0, i) for i in range(a)]
    f += [wide(dlo_ref, a, i) + wide(lo_ref, 0, i) for i in range(a)]
    f += [wide(dlo_ref, b, i) + wide(lo_ref, a, i) + wide(p_ref, 0, i) for i in range(a)]
    f += [f_ref[i] for i in range(a)]
    f += [wide(dhi_ref, b, i) + wide(hi_ref, a, i) + wide(p_ref, b, i) for i in range(a)]
    f += [wide(dhi_ref, a, i) + wide(hi_ref, b, i) for i in range(a)]
    f += [wide(dhi_ref, 0, i) for i in range(a)]
    count = len(f)
    inv = [damping / g for g in diagonal]
    start = [f[i] * inv[i] for i in range(count)]
    for i in range(count):
        v0_ref[i] = start[i].astype(bf16)
    x1 = []
    for j in range(count - 4):
        p = product(v0_ref, [j + c for c in columns(j)], weights(j))
        x1.append(1.2 * start[j + 2] + inv[j + 2] * p)
        v1_ref[j] = x1[j].astype(bf16)
    res = []
    x2 = []
    for j in range(count - 8):
        p = product(v1_ref, [j + c for c in columns(j + 2)], weights(j + 2))
        r = f[j + 4] - diagonal[j + 4] * x1[j + 2] + p
        res.append(r)
        x2.append(x1[j + 2] + inv[j + 4] * r)
        v2_ref[j] = x2[j].astype(bf16)
    left = []
    right = []
    for d in (-1, 0, 1):
        r = jnp.concatenate(res[(d + 1) * a : (d + 2) * a], axis=1)
        left.append(jnp.where(row(d, 0) == -d, r, 0.0).astype(bf16))
        rows = lax.broadcasted_iota(i32, (C3, NB2 * BS), 0)
        right.append(jnp.where(rows == row(d, 1), 1.0, 0.0).astype(bf16))
    c = lax.dot_general(
        jnp.concatenate(left, axis=1), jnp.concatenate(right, axis=1),
        (((1,), (1,)), ((), ())), preferred_element_type=f32,
    ).astype(bf16)
    for i in range(c_ref.shape[0]):
        c_ref[i] = c
    for i in range(a):
        p = product(v2_ref, [i + c for c in columns(i + 4)], weights(i + 4))
        z_ref[i] = 0.2 * x2[i + 2] + start[i + 6] + inv[i + 6] * p


def third_down(copies, *args):
    count = 2 * NB2 * REACH + NB2
    return call(
        third_down_kernel, "down2",
        (shape((copies, R, C3), bf16), shape((NB2, R, BS), f32)),
        [vmem()] * 12, (vmem(),) * 2,
        [
            pltpu.VMEM((count, R, BS), bf16), pltpu.VMEM((count - 4, R, BS), bf16), pltpu.VMEM((count - 8, R, BS), bf16)
        ],
        mib=12, flops=2**27, nbytes=2**21,
    )(*args)


def coarse_kernel(got_ref, z_ref, s_ref, out_ref, copy_ref):
    count = got_ref.shape[0]
    chunks = 4
    size = count // chunks
    u = jnp.zeros((R, C3), f32)
    for c in range(chunks):
        u = u + lax.dot_general(
            joined(got_ref, range(c * size, (c + 1) * size)), s_ref[:, c * size * BS : (c + 1) * size * BS],
            (((1,), (1,)), ((), ())), preferred_element_type=f32,
        )
    out_ref[0] = u.astype(bf16)
    out_ref[1:] = z_ref[...].astype(bf16)
    copy_ref[...] = out_ref[...]


def coarse_solve(got, z, inverse_rows):
    count = got.shape[0]
    return call(
        coarse_kernel, "coarse", (shape((1 + NB2, R, BS), bf16),) * 2,
        [vmem()] * 3, (vmem(),) * 2,
        flops=2**26, nbytes=2**21,
    )(got, z, inverse_rows)


def three_kernel(lo_ref, own_ref, hi_ref, out_ref, copy_ref):
    out_ref[0] = lo_ref[0]
    out_ref[1] = own_ref[0]
    out_ref[2] = hi_ref[0]
    copy_ref[...] = out_ref[...]


def three_of(lo, own, hi):
    return call(
        three_kernel, "three", (shape((3, R, BS), bf16),) * 2, [vmem()] * 3, (vmem(),) * 2,
        flops=2**15, nbytes=2**16,
    )(lo, own, hi)


def third_up_kernel(
    own_ref, lo_ref, hi_ref, ulo_ref, uhi_ref, z_ref, w3_ref, tail_ref, slo_ref, shi_ref, rlo_ref, rhi_ref,
    own2_ref, slot2_ref, x_ref,
    out_ref, first_ref, last_ref,
    v0_ref, v1_ref, e_ref,
):
    diagonal, weights, columns, row = third_fixed(w3_ref, tail_ref, slo_ref, shi_ref, rlo_ref, rhi_ref)
    inv = [damping / g for g in diagonal]
    u = [ulo_ref[0], ulo_ref[1], ulo_ref[2], lo_ref[0], own_ref[0], hi_ref[0], uhi_ref[0], uhi_ref[1], uhi_ref[2]]
    y = []
    for d in range(-REACH, REACH + 1):
        rows = lax.broadcasted_iota(i32, (C3, NB2 * BS), 0)
        pick = jnp.where(rows == row(d, 1), 1.0, 0.0).astype(bf16)
        at = d + REACH
        found = jnp.dot(jnp.concatenate(u[at : at + 3], axis=0), pick, preferred_element_type=f32)
        owner = row(d, 0)
        got = jnp.zeros((R, NB2 * BS), f32)
        for i in range(3):
            got = got + jnp.where(owner == i - 1, found[i * R : (i + 1) * R], 0.0)
        y += [got[:, i * BS : (i + 1) * BS] for i in range(NB2)]
    count = len(y)
    for i in range(count):
        v0_ref[i] = y[i].astype(bf16)
    y1 = []
    for j in range(count - 4):
        p = product(v0_ref, [j + c for c in columns(j)], weights(j))
        y1.append(0.2 * y[j + 2] + inv[j + 2] * p)
        v1_ref[j] = y1[j].astype(bf16)
    for j in range(count - 8):
        p = product(v1_ref, [j + c for c in columns(j + 2)], weights(j + 2))
        y2 = 0.2 * y1[j + 2] + inv[j + 4] * p
        i = j % NB2
        z = (lambda: lo_ref[1 + i].astype(f32), lambda: z_ref[i], lambda: hi_ref[1 + i].astype(f32))[j // NB2]()
        place(e_ref, j, (z + y2).astype(bf16))
    spread(NB1, NB2, e_ref, own2_ref, slot2_ref, device_index(), x_ref, out_ref)
    first_ref[...] = out_ref[:EDGE].astype(bf16)
    last_ref[...] = out_ref[NB1 - EDGE :].astype(bf16)


def third_up(*args):
    count = 2 * NB2 * REACH + NB2
    return call(
        third_up_kernel, "up2",
        (shape((NB1, R, BS), f32), shape((EDGE, R, BS), bf16), shape((EDGE, R, BS), bf16)),
        [vmem()] * 15, (vmem(),) * 3,
        [
            pltpu.VMEM((count, R, BS), bf16), pltpu.VMEM((count - 4, R, BS), bf16),
            pltpu.VMEM((3 * NB2 // 2 * R, 2 * BS), bf16),
        ],
        mib=12, flops=2**27, nbytes=2**21,
    )(*args)


def on_device(
    right_sides,
    weights_fine, columns_fine, degree_fine, owners_fine, slots_fine,
    weights_second, columns_second, degree_second, owners_second, slots_second,
    weights_third, columns_third, degree_third, owners_third, slots_third,
    coarse_inverse,
):
    flat = lambda a: a.reshape(-1, BS)
    f = right_sides
    columns_fine, columns_second, columns_third = columns_fine.T, columns_second.T, columns_third.T
    w1, w2, w3 = (in_hbm(flat(w)) for w in (weights_fine, weights_second, weights_third))
    edges1 = both_ways(*first_edges(in_hbm(flat(f)), w1, in_hbm(degree_fine), in_hbm(columns_fine)))
    g1, g2, _, up, down, w3, tail, kept1 = fixed_data(
        w1, w2, w3, degree_fine, degree_second, degree_third, columns_second, columns_third, owners_third, slots_third
    )
    fixed = both_ways(up, down)
    far = both_ways(*far_data(w3, tail, *fixed), 2)
    third = (w3, tail, *fixed, *far)

    inner = inner_sweep(NB0, True, columns_fine, f, f, g1, kept1)
    x1, low, mid, high = go_down(
        NB0, NB1, F_ROWS, columns_fine, f, g1, owners_fine, slots_fine, edges1, edges1, kept1, 20, inner
    )
    lo, hi = both_ways(high, low)
    f2, up, down = second_rhs(mid, lo, hi)
    f_edges = both_ways(up, down)
    x2, low, mid, high = go_down(
        NB1, NB2, 0, columns_second, f2, g2, owners_second, slots_second, f_edges, fixed, w2, 12
    )
    parts, copy = parts_of(low, mid, high)
    plo, phi = both_ways(copy, parts)
    f3, up, down = third_window(mid, parts, plo, phi)
    dlo, dhi = both_ways(up, down, 3)
    c, z = third_down(lax.axis_size("col"), f3, parts, plo, phi, dlo, dhi, *third)
    got = lax.all_to_all(c, "col", 0, 0, tiled=True)
    own, copy = coarse_solve(got, z, coarse_inverse)
    lo, hi = both_ways(copy, own)
    near, copy = three_of(lo, own, hi)
    ulo, uhi = both_ways(near, copy, 3)
    x2, first, last = third_up(own, lo, hi, ulo, uhi, z, *third, owners_second, slots_second, x2)
    x_edges = both_ways(last, first)
    x2, copy = go_up(NB1, 0, columns_second, x2, x_edges, f2, g2, f_edges, fixed, w2, bf16, 12, 2)
    lo, hi = both_ways(copy, x2)
    x1, first, last = prolong(NB0, NB1, owners_fine, slots_fine, lo, x2, hi, x1)
    x_edges = both_ways(last, first)
    inner = inner_sweep(NB0, False, columns_fine, x1, f, g1, kept1)
    return go_up(NB0, F_ROWS, columns_fine, x1, x_edges, f, g1, edges1, edges1, kept1, f32, 20, 1, inner)[0]


def solution(mesh):
    block = P(AXES, None, None)
    pair = P(AXES, None)
    four = P(AXES, None, None, None)
    level = (four, pair, pair, pair, pair)
    return jax.shard_map(
        on_device, mesh=mesh, in_specs=(block, *level, *level, *level, pair), out_specs=block, check_vma=False
    )
```

```python
import functools

import jax
import jax.numpy as jnp
from jax import lax
from jax.experimental import pallas as pl
from jax.experimental.pallas import tpu as pltpu
from jax.sharding import PartitionSpec as P

BS = 128
R = 64
K = 3
HB = 2
NB2 = 2
NB1 = 8
NB0 = 32
C3 = 128
AXES = ("row", "col")
EDGE = 2 * HB
ROWS = K * BS
damping = 0.8
bf16 = jnp.bfloat16
f32 = jnp.float32
i32 = jnp.int32
INV = 1.0 / (K * BS)

F_ROWS = EDGE * R
W_ROWS = HB * ROWS
TAIL = 16
EDGE1 = F_ROWS + W_ROWS + TAIL
EDGE2 = W_ROWS + TAIL
THIRD = NB2 * ROWS + TAIL
FIXED = EDGE2 + THIRD
FAR = NB2 * ROWS + 3 * TAIL


def passed_along(value, steps):
    count = lax.axis_size(AXES)
    return lax.ppermute(value, AXES, [(s, (s + steps) % count) for s in range(count)])


def both_ways(up, down, steps=1):
    return passed_along(up, steps), passed_along(down, -steps)


def in_hbm(x):
    return pltpu.with_memory_space_constraint(x, pltpu.HBM)


def vmem():
    return pl.BlockSpec(memory_space=pltpu.VMEM)


def smem():
    return pl.BlockSpec(memory_space=pltpu.SMEM)


def hbm():
    return pl.BlockSpec(memory_space=pltpu.HBM)


def shape(dims, dtype):
    return jax.ShapeDtypeStruct(dims, dtype)


def call(kernel, name, outs, in_specs, out_specs, scratch=(), mib=6, flops=0, nbytes=0):
    return pl.pallas_call(
        kernel,
        out_shape=outs,
        in_specs=in_specs,
        out_specs=out_specs,
        scratch_shapes=list(scratch),
        compiler_params=pltpu.CompilerParams(vmem_limit_bytes=mib * 1024 * 1024),
        cost_estimate=pl.CostEstimate(flops=flops, transcendentals=0, bytes_accessed=nbytes),
        name=name,
    )


def device_index():
    return lax.axis_index(AXES)


def near_row(values):
    lane = lax.broadcasted_iota(i32, (1, BS), 1)
    row = jnp.zeros((1, BS), f32)
    for i, v in enumerate(values):
        row = jnp.where(lane == i, v.astype(f32), row)
    return row


def read_near(row):
    lane = lax.broadcasted_iota(i32, (1, BS), 1)
    row = row.astype(f32)
    return [jnp.sum(jnp.where(lane == i, row, 0.0)).astype(i32) for i in range(HB * K)]


def near_of(col_ref, first, b, k):
    return col_ref[k, b] - (first + b - HB)


def column_sum(w):
    return jnp.sum(w.astype(f32), axis=0, keepdims=True)


def diagonal_rows(ref, at, stride, i):
    return ref[at + i : at + i + 1, :].astype(f32) + ref[at + stride + i : at + stride + i + 1, :].astype(f32)


def inverse(g):
    return jnp.where(g > 0, damping / g, 0.0)


def joined(v_ref, indices):
    return jnp.concatenate([v_ref[i] for i in indices], axis=1)


def product(v_ref, indices, w):
    return jnp.dot(joined(v_ref, indices), w, preferred_element_type=f32) * INV


def tail_rows(gs, nears, extra=()):
    high = [g.astype(bf16).astype(f32) for g in gs]
    low = [g - h for g, h in zip(gs, high)]
    rows = high + low + [near_row(nears)] + list(extra)
    rows = rows + [jnp.zeros((1, BS), f32)] * (TAIL - len(rows))
    return jnp.concatenate(rows, axis=0).astype(bf16)


def edge_kernel(f_hbm, w_hbm, deg_hbm, col_hbm, up_ref, down_ref, w_ref, deg_ref, col_ref, sem):
    n = NB0
    small = [
        pltpu.make_async_copy(deg_hbm, deg_ref, sem.at[6]),
        pltpu.make_async_copy(col_hbm, col_ref, sem.at[7]),
    ]
    first = device_index() * n
    copies = [
        pltpu.make_async_copy(w_hbm.at[pl.ds((n - EDGE) * ROWS, EDGE * ROWS)], w_ref.at[1], sem.at[0]),
        pltpu.make_async_copy(w_hbm.at[pl.ds(0, EDGE * ROWS)], w_ref.at[0], sem.at[1]),
        pltpu.make_async_copy(f_hbm.at[pl.ds((n - EDGE) * R, F_ROWS)], up_ref.at[pl.ds(0, F_ROWS)], sem.at[2]),
        pltpu.make_async_copy(f_hbm.at[pl.ds(0, F_ROWS)], down_ref.at[pl.ds(0, F_ROWS)], sem.at[3]),
        pltpu.make_async_copy(
            w_hbm.at[pl.ds((n - HB) * ROWS, W_ROWS)], up_ref.at[pl.ds(F_ROWS, W_ROWS)], sem.at[4]
        ),
        pltpu.make_async_copy(w_hbm.at[pl.ds(0, W_ROWS)], down_ref.at[pl.ds(F_ROWS, W_ROWS)], sem.at[5]),
    ]
    for c in small + copies:
        c.start()
    for c in small:
        c.wait()
    for side, ref, start, near_start in ((1, up_ref, n - EDGE, n - HB), (0, down_ref, 0, 0)):
        copies[1 - side].wait()
        gs = [
            deg_ref[start + i : start + i + 1, :] + column_sum(w_ref[side, i * ROWS : (i + 1) * ROWS, :]) * INV
            for i in range(EDGE)
        ]
        nears = [near_of(col_ref, first, near_start + i, k) for i in range(HB) for k in range(K)]
        ref[F_ROWS + W_ROWS :, :] = tail_rows(gs, nears)
    for c in copies[2:]:
        c.wait()


def first_edges(f, w, deg, col):
    return call(
        edge_kernel, "edges",
        (shape((EDGE1, BS), bf16),) * 2,
        [hbm()] * 4,
        (vmem(),) * 2,
        [
            pltpu.VMEM((2, EDGE * ROWS, BS), bf16),
            pltpu.VMEM((NB0, BS), f32),
            pltpu.SMEM((K, NB0), i32),
            pltpu.SemaphoreType.DMA((8,)),
        ],
        flops=2**20, nbytes=2**21,
    )(f, w, deg, col)


def fixed_kernel(
    w1_hbm, w2_hbm, w3_hbm, deg1_ref, deg2_ref, deg3_ref, col2_ref, col3_ref, own3_ref, slot3_ref,
    g1_ref, g2_ref, g3_ref, up_ref, down_ref, w3_ref, tail_ref, w1_ref, w2_ref, sem,
):
    device = device_index()
    chunks = 4
    size = NB0 // chunks
    last3 = pltpu.make_async_copy(w3_hbm, w3_ref, sem.at[0])
    last2 = pltpu.make_async_copy(w2_hbm, w2_ref, sem.at[1])
    copies = [
        pltpu.make_async_copy(
            w2_hbm.at[pl.ds((NB1 - HB) * ROWS, W_ROWS)], up_ref.at[pl.ds(0, W_ROWS)], sem.at[2]
        ),
        pltpu.make_async_copy(w2_hbm.at[pl.ds(0, W_ROWS)], down_ref.at[pl.ds(0, W_ROWS)], sem.at[3]),
        pltpu.make_async_copy(w3_hbm, up_ref.at[pl.ds(EDGE2, W_ROWS)], sem.at[4]),
        pltpu.make_async_copy(w3_hbm, down_ref.at[pl.ds(EDGE2, W_ROWS)], sem.at[5]),
    ]
    bulk = [
        pltpu.make_async_copy(
            w1_hbm.at[pl.ds(c * size * ROWS, size * ROWS)], w1_ref.at[pl.ds(c * size * ROWS, size * ROWS)], sem.at[6 + c]
        )
        for c in range(chunks)
    ]
    for c in [last3, last2] + copies + bulk:
        c.start()
    last3.wait()
    g3 = [deg3_ref[i : i + 1, :] + column_sum(w3_ref[i * ROWS : (i + 1) * ROWS, :]) * INV for i in range(NB2)]
    for i in range(NB2):
        g3_ref[i : i + 1, :] = g3[i]
    nears = [near_of(col3_ref, device * NB2, i, k) for i in range(NB2) for k in range(K)]
    extra = [(own3_ref[i : i + 1, :] - device).astype(f32) for i in range(NB2)]
    extra = extra + [slot3_ref[i : i + 1, :].astype(f32) for i in range(NB2)]
    tail = tail_rows(g3, nears, extra)
    tail_ref[...] = tail
    up_ref[EDGE2 + W_ROWS :, :] = tail
    down_ref[EDGE2 + W_ROWS :, :] = tail
    last2.wait()
    g2 = [deg2_ref[i : i + 1, :] + column_sum(w2_ref[i * ROWS : (i + 1) * ROWS, :]) * INV for i in range(NB1)]
    for i in range(NB1):
        g2_ref[i : i + 1, :] = g2[i]
    first = device * NB1
    up_ref[W_ROWS : W_ROWS + TAIL, :] = tail_rows(
        g2[NB1 - EDGE :], [near_of(col2_ref, first, NB1 - HB + i, k) for i in range(HB) for k in range(K)]
    )
    down_ref[W_ROWS : W_ROWS + TAIL, :] = tail_rows(
        g2[:EDGE], [near_of(col2_ref, first, i, k) for i in range(HB) for k in range(K)]
    )

    def one(b, carry):
        at = pl.multiple_of(b * ROWS, ROWS)
        g1_ref[pl.ds(b, 1), :] = deg1_ref[pl.ds(b, 1), :] + column_sum(w1_ref[pl.ds(at, ROWS), :]) * INV
        return carry

    for c in range(chunks):
        bulk[c].wait()
        lax.fori_loop(c * size, (c + 1) * size, one, 0, unroll=2)
    for c in copies:
        c.wait()


def fixed_data(w1, w2, w3, deg1, deg2, deg3, col2, col3, own3, slot3):
    return call(
        fixed_kernel, "fixed",
        (
            shape((NB0, BS), f32), shape((NB1, BS), f32), shape((NB2, BS), f32),
            shape((FIXED, BS), bf16), shape((FIXED, BS), bf16),
            shape((NB2 * ROWS, BS), bf16), shape((TAIL, BS), bf16), shape((NB0 * ROWS, BS), bf16),
            shape((NB1 * ROWS, BS), bf16),
        ),
        [hbm()] * 3 + [vmem()] * 3 + [smem()] * 2 + [vmem()] * 2,
        (vmem(),) * 9,
        [pltpu.SemaphoreType.DMA((10,))],
        mib=10, flops=2**30, nbytes=2**22,
    )(w1, w2, w3, deg1, deg2, deg3, col2, col3, own3, slot3)


def far_kernel(w3_ref, tail_ref, lo_ref, hi_ref, out_ref, copy_ref):
    at = NB2 * ROWS
    out_ref[:at, :] = w3_ref[...]
    out_ref[at : at + TAIL, :] = lo_ref[FIXED - TAIL :, :]
    out_ref[at + TAIL : at + 2 * TAIL, :] = tail_ref[...]
    out_ref[at + 2 * TAIL :, :] = hi_ref[FIXED - TAIL :, :]
    copy_ref[...] = out_ref[...]


def far_data(w3, tail, lo, hi):
    return call(
        far_kernel, "far", (shape((FAR, BS), bf16),) * 2, [vmem()] * 4, (vmem(),) * 2, flops=2**20, nbytes=2**19
    )(w3, tail, lo, hi)


def weight_copies(w_hbm, w_ref, sem, n, chunks):
    size = n // chunks * ROWS
    return [
        pltpu.make_async_copy(w_hbm.at[pl.ds(c * size, size)], w_ref.at[pl.ds(c * size, size)], sem.at[c])
        for c in range(chunks)
    ]


def weight_of(w_ref, b):
    return w_ref[pl.ds(pl.multiple_of(b * ROWS, ROWS), ROWS), :]


def edge_starts(base, f_ref, s_ref):
    if base:
        rhs = lambda i: f_ref[i * R : (i + 1) * R, :].astype(f32)
    else:
        rhs = lambda i: f_ref[i].astype(f32)
    inv = [inverse(diagonal_rows(s_ref, base + W_ROWS, EDGE, i)) for i in range(EDGE)]
    return rhs, inv


def down_kernel(
    n, nc, base, chunks,
    col_ref, f_ref, g_ref, own_ref, slot_ref, flo_ref, fhi_ref, slo_ref, shi_ref, *rest,
):
    inner_ref = None
    if chunks:
        w_hbm, x_ref, down_ref, mid_ref, up_ref, v0_ref, v1_ref, r_ref, acc_ref, w_ref, sem = rest
        copies = weight_copies(w_hbm, w_ref, sem, n, chunks)
        for c in copies:
            c.start()
        size = n // chunks
    else:
        w_ref, inner_ref, x_ref, down_ref, mid_ref, up_ref, v0_ref, v1_ref, r_ref, acc_ref = rest
    device = device_index()
    start = device * n

    def scale(b):
        return damping / g_ref[pl.ds(b, 1), :]

    def fill(b, carry):
        v0_ref[b + EDGE] = (f_ref[b].astype(f32) * scale(b)).astype(bf16)
        return carry

    lax.fori_loop(0, n, fill, 0, unroll=2)
    sides = []
    for side, fr, sr in ((0, flo_ref, slo_ref), (1, fhi_ref, shi_ref)):
        rhs, inv = edge_starts(base, fr, sr)
        starts = [rhs(i) * inv[i] for i in range(EDGE)]
        for i in range(EDGE):
            v0_ref[i + side * (n + EDGE)] = starts[i].astype(bf16)
        near = read_near(sr[base + W_ROWS + 2 * EDGE : base + W_ROWS + 2 * EDGE + 1, :])
        sides.append((side, sr, starts, inv, near))
    for side, sr, starts, inv, near in sides:
        for i in range(HB):
            e = i + HB * (1 - side)
            j = i + side * (n + HB)
            w = sr[base + i * ROWS : base + (i + 1) * ROWS, :]
            p = product(v0_ref, [j + near[i * K + k] for k in range(K)], w)
            v1_ref[j] = (1.2 * starts[e] + inv[e] * p).astype(bf16)

    def first(b, carry):
        p = product(v0_ref, [b + HB + near_of(col_ref, start, b, k) for k in range(K)], weight_of(w_ref, b))
        s = scale(b)
        x = 1.2 * (f_ref[b].astype(f32) * s) + s * p
        x_ref[b] = x
        v1_ref[b + HB] = x.astype(bf16)
        return carry

    for c in range(chunks):
        copies[c].wait()
        lax.fori_loop(c * size, (c + 1) * size, first, 0, unroll=4 if size % 4 == 0 else 2)
    if not chunks:
        take_inner(n, inner_ref, x_ref, v1_ref)
        for b in edge_blocks(n):
            first(b, 0)

    def residual(b):
        p = product(v1_ref, [b + near_of(col_ref, start, b, k) for k in range(K)], weight_of(w_ref, b))
        return f_ref[b].astype(f32) - g_ref[pl.ds(b, 1), :] * x_ref[b] + p

    def second(q, carry):
        r_ref[q] = jnp.concatenate([residual(2 * q), residual(2 * q + 1)], axis=1).astype(bf16)
        return carry

    lax.fori_loop(0, n // 2, second, 0, unroll=2)

    highs = 3 * nc // 2
    group = 4
    acc_ref[...] = jnp.zeros_like(acc_ref)

    def gather(q, carry):
        left = []
        right = []
        for i in range(group):
            t = pair_targets(own_ref, slot_ref, device, nc, q * group + i)
            r = r_ref[q * group + i]
            high = t // 256
            left.append(
                jnp.concatenate([r * jnp.where(high == h, 1.0, 0.0).astype(bf16) for h in range(highs)], axis=0)
            )
            rows = lax.broadcasted_iota(i32, (256, 256), 0)
            right.append(jnp.where(rows == t % 256, 1.0, 0.0).astype(bf16))
        acc_ref[...] += lax.dot_general(
            jnp.concatenate(left, axis=1),
            jnp.concatenate(right, axis=1),
            (((1,), (1,)), ((), ())),
            preferred_element_type=f32,
        )
        return carry

    lax.fori_loop(0, n // 2 // group, gather, 0)

    for b in range(3 * nc):
        part = acc_ref[(b // 2) * R : (b // 2 + 1) * R, (b % 2) * BS : (b % 2 + 1) * BS]
        where = b // nc
        ref = (down_ref, mid_ref, up_ref)[where]
        ref[b - where * nc] = part.astype(ref.dtype)


def edge_blocks(n):
    return list(range(HB)) + list(range(n - HB, n))


def take_inner(n, inner_ref, x_ref, v_ref):
    def one(b, carry):
        x = inner_ref[b]
        x_ref[b] = x
        v_ref[b + HB] = x.astype(bf16)
        return carry

    lax.fori_loop(HB, n - HB, one, 0, unroll=4)


def pair_targets(own_ref, slot_ref, device, nc, q):
    row = lambda b: (own_ref[pl.ds(b, 1), :] - device + 1) * (nc * BS) + slot_ref[pl.ds(b, 1), :]
    return jnp.concatenate([row(2 * q), row(2 * q + 1)], axis=1)


def go_down(n, nc, base, col, f, g, own, slot, f_edges, fixed, weights, mib, inner=None):
    chunks = 0 if inner is not None else 4
    loads = [pltpu.VMEM((n * ROWS, BS), bf16), pltpu.SemaphoreType.DMA((4,))] if chunks else []
    last = (weights,) if chunks else (weights, inner)
    highs = 3 * nc // 2
    return call(
        functools.partial(down_kernel, n, nc, base, chunks), f"down{n}",
        (
            shape((n, R, BS), f32), shape((nc, R, BS), bf16), shape((nc, R, BS), f32), shape((nc, R, BS), bf16)
        ),
        [smem()] + [vmem()] * 8 + ([hbm()] if chunks else [vmem()] * 2),
        (vmem(),) * 4,
        [
            pltpu.VMEM((n + 2 * EDGE, R, BS), bf16),
            pltpu.VMEM((n + EDGE, R, BS), bf16),
            pltpu.VMEM((n // 2, R, 2 * BS), bf16),
            pltpu.VMEM((highs * R, 2 * BS), f32),
            *loads,
        ],
        mib=mib, flops=4 * n * R * ROWS * BS, nbytes=n * ROWS * BS * 2,
    )(col, f, g, own, slot, *f_edges, *fixed, *last)


def rhs_kernel(mid_ref, lo_ref, hi_ref, out_ref, up_ref, down_ref):
    out_ref[...] = mid_ref[...] + lo_ref[...].astype(f32) + hi_ref[...].astype(f32)
    up_ref[...] = out_ref[NB1 - EDGE :].astype(bf16)
    down_ref[...] = out_ref[:EDGE].astype(bf16)


def second_rhs(mid, lo, hi):
    return call(
        rhs_kernel, "rhs8",
        (shape((NB1, R, BS), f32), shape((EDGE, R, BS), bf16), shape((EDGE, R, BS), bf16)),
        [vmem()] * 3, (vmem(),) * 3, flops=2**18, nbytes=2**19,
    )(mid, lo, hi)


def spread(n, nc, e_ref, own_ref, slot_ref, device, x_ref, out_ref):
    highs = 3 * nc // 2

    def step(q, carry):
        t = pair_targets(own_ref, slot_ref, device, nc, q)
        rows = lax.broadcasted_iota(i32, (256, 256), 0)
        pick = jnp.where(rows == t % 256, 1.0, 0.0).astype(bf16)
        found = jnp.dot(e_ref[...], pick, preferred_element_type=f32)
        high = t // 256
        y = jnp.zeros((R, 256), f32)
        for h in range(highs):
            y = y + jnp.where(high == h, found[h * R : (h + 1) * R], 0.0)
        out_ref[2 * q] = x_ref[2 * q] + y[:, :BS]
        out_ref[2 * q + 1] = x_ref[2 * q + 1] + y[:, BS:]
        return carry

    lax.fori_loop(0, n // 2, step, 0, unroll=2)


def place(e_ref, b, value):
    e_ref[(b // 2) * R : (b // 2 + 1) * R, (b % 2) * BS : (b % 2 + 1) * BS] = value


def prolong_kernel(
    n, nc, own_ref, slot_ref, lo_ref, mid_ref, hi_ref, x_ref, out_ref, first_ref, last_ref, e_ref
):
    for b in range(3 * nc):
        place(e_ref, b, (lo_ref, mid_ref, hi_ref)[b // nc][b % nc])
    spread(n, nc, e_ref, own_ref, slot_ref, device_index(), x_ref, out_ref)
    first_ref[...] = out_ref[:EDGE].astype(bf16)
    last_ref[...] = out_ref[n - EDGE :].astype(bf16)


def prolong(n, nc, own, slot, lo, mid, hi, x):
    return call(
        functools.partial(prolong_kernel, n, nc), f"prolong{n}",
        (shape((n, R, BS), f32), shape((EDGE, R, BS), bf16), shape((EDGE, R, BS), bf16)),
        [vmem()] * 6,
        (vmem(),) * 3,
        [pltpu.VMEM((3 * nc // 2 * R, 2 * BS), bf16)],
        mib=12, flops=2 * n * BS * 3 * nc * BS * R, nbytes=2 * n * R * BS * 4,
    )(own, slot, lo, mid, hi, x)


def up_kernel(
    n, base, chunks,
    col_ref, x_ref, xlo_ref, xhi_ref, f_ref, g_ref, flo_ref, fhi_ref, slo_ref, shi_ref, w_ref, *rest,
):
    inner_ref = None
    if chunks:
        *outs, v0_ref, v1_ref, keep_ref, kept_ref, sem = rest
        copies = weight_copies(w_ref, kept_ref, sem, n, chunks)
        w_ref = kept_ref
        for c in copies:
            c.start()
        size = n // chunks
    else:
        inner_ref, *outs, v0_ref, v1_ref, keep_ref = rest
    out_ref = outs[0]
    start = device_index() * n

    def fill(b, carry):
        v0_ref[b + EDGE] = x_ref[b].astype(bf16)
        return carry

    lax.fori_loop(0, n, fill, 0, unroll=2)
    v0_ref[:EDGE] = xlo_ref[...]
    v0_ref[n + EDGE :] = xhi_ref[...]
    sides = []
    for side, fr, sr, xr in ((0, flo_ref, slo_ref, xlo_ref), (1, fhi_ref, shi_ref, xhi_ref)):
        near = read_near(sr[base + W_ROWS + 2 * EDGE : base + W_ROWS + 2 * EDGE + 1, :])
        sides.append((side, sr, xr, *edge_starts(base, fr, sr), near))
    for side, sr, xr, rhs, inv, near in sides:
        for i in range(HB):
            e = i + HB * (1 - side)
            j = i + side * (n + HB)
            w = sr[base + i * ROWS : base + (i + 1) * ROWS, :]
            p = product(v0_ref, [j + near[i * K + k] for k in range(K)], w)
            v1_ref[j] = (0.2 * xr[e].astype(f32) + inv[e] * (rhs(e) + p)).astype(bf16)

    def sweep(b, x, p):
        return 0.2 * x + (damping / g_ref[pl.ds(b, 1), :]) * (f_ref[b].astype(f32) + p)

    def near(b, base):
        return [b + base + near_of(col_ref, start, b, k) for k in range(K)]

    def first(b, carry):
        x = sweep(b, x_ref[b], product(v0_ref, near(b, HB), weight_of(w_ref, b)))
        keep_ref[b] = x
        v1_ref[b + HB] = x.astype(bf16)
        return carry

    for c in range(chunks):
        copies[c].wait()
        lax.fori_loop(c * size, (c + 1) * size, first, 0, unroll=4 if size % 4 == 0 else 2)
    if not chunks:
        take_inner(n, inner_ref, keep_ref, v1_ref)
        for b in edge_blocks(n):
            first(b, 0)

    def second(b, carry):
        p = product(v1_ref, near(b, 0), weight_of(w_ref, b))
        x = sweep(b, keep_ref[b], p).astype(out_ref.dtype)
        for ref in outs:
            ref[b] = x
        return carry

    lax.fori_loop(0, n, second, 0, unroll=4)


def go_up(n, base, col, x, x_edges, f, g, f_edges, fixed, weights, dtype, mib, outs=1, inner=None):
    chunks = 0 if inner is not None else 4
    loads = [pltpu.VMEM((n * ROWS, BS), bf16), pltpu.SemaphoreType.DMA((4,))] if chunks else []
    last = (weights,) if chunks else (weights, inner)
    return call(
        functools.partial(up_kernel, n, base, chunks), f"up{n}",
        (shape((n, R, BS), dtype),) * outs,
        [smem()] + [vmem()] * 9 + ([hbm()] if chunks else [vmem()] * 2),
        (vmem(),) * outs,
        [
            pltpu.VMEM((n + 2 * EDGE, R, BS), bf16),
            pltpu.VMEM((n + EDGE, R, BS), bf16),
            pltpu.VMEM((n, R, BS), f32),
            *loads,
        ],
        mib=mib, flops=4 * n * R * ROWS * BS, nbytes=n * ROWS * BS * 2,
    )(col, x, *x_edges, f, g, *f_edges, *fixed, *last)


def inner_kernel(n, first_sweep, col_ref, x_ref, f_ref, g_ref, w_ref, out_ref, v_ref):
    start = device_index() * n

    def scale(b):
        return damping / g_ref[pl.ds(b, 1), :]

    def fill(b, carry):
        x = f_ref[b].astype(f32) * scale(b) if first_sweep else x_ref[b]
        v_ref[b] = x.astype(bf16)
        return carry

    lax.fori_loop(0, n, fill, 0, unroll=4)

    def one(b, carry):
        p = product(v_ref, [b - HB + near_of(col_ref, start, b, k) for k in range(K)], weight_of(w_ref, b))
        s = scale(b)
        f = f_ref[b].astype(f32)
        out_ref[b] = 1.2 * (f * s) + s * p if first_sweep else 0.2 * x_ref[b] + s * (f + p)
        return carry

    lax.fori_loop(HB, n - HB, one, 0, unroll=4)
    blank = jnp.zeros((R, BS), f32)
    for b in list(range(HB)) + list(range(n - HB, n)):
        out_ref[b] = blank


def inner_sweep(n, first_sweep, col, x, f, g, w):
    return call(
        functools.partial(inner_kernel, n, first_sweep), "inner" + ("down" if first_sweep else "up") + str(n),
        shape((n, R, BS), f32),
        [smem()] + [vmem()] * 4, vmem(), [pltpu.VMEM((n, R, BS), bf16)],
        mib=12, flops=2 * n * R * ROWS * BS, nbytes=2**20,
    )(col, x, f, g, w)


def parts_kernel(low_ref, mid_ref, high_ref, out_ref, copy_ref):
    out_ref[:NB2] = low_ref[...]
    out_ref[NB2 : 2 * NB2] = mid_ref[...].astype(bf16)
    out_ref[2 * NB2 :] = high_ref[...]
    copy_ref[...] = out_ref[...]


def parts_of(low, mid, high):
    return call(
        parts_kernel, "parts", (shape((3 * NB2, R, BS), bf16),) * 2, [vmem()] * 3, (vmem(),) * 2,
        flops=2**17, nbytes=2**17,
    )(low, mid, high)


def window_kernel(mid_ref, p_ref, lo_ref, hi_ref, f_ref, up_ref, down_ref):
    a, b = NB2, 2 * NB2
    f_ref[...] = mid_ref[...] + lo_ref[b:].astype(f32) + hi_ref[:a].astype(f32)
    own = f_ref[...].astype(bf16)
    up_ref[:a] = own
    up_ref[a:b] = (hi_ref[a:b].astype(f32) + p_ref[b:].astype(f32)).astype(bf16)
    up_ref[b:] = hi_ref[b:]
    down_ref[:a] = own
    down_ref[a:b] = (lo_ref[a:b].astype(f32) + p_ref[:a].astype(f32)).astype(bf16)
    down_ref[b:] = lo_ref[:a]


def third_window(mid, p, lo, hi):
    return call(
        window_kernel, "window",
        (shape((NB2, R, BS), f32), shape((3 * NB2, R, BS), bf16), shape((3 * NB2, R, BS), bf16)),
        [vmem()] * 4, (vmem(),) * 3, flops=2**18, nbytes=2**18,
    )(mid, p, lo, hi)


REACH = 3


def third_fixed(w3_ref, tail_ref, slo_ref, shi_ref, rlo_ref, rhi_ref):
    at = NB2 * ROWS
    tails = {0: (tail_ref, 0), -1: (slo_ref, FIXED - TAIL), 1: (shi_ref, FIXED - TAIL)}
    tails[-3], tails[-2] = (rlo_ref, at), (rlo_ref, at + TAIL)
    tails[2], tails[3] = (rhi_ref, at + TAIL), (rhi_ref, at + 2 * TAIL)
    matrices = {0: (w3_ref, 0), -1: (slo_ref, EDGE2), 1: (shi_ref, EDGE2), -2: (rlo_ref, 0), 2: (rhi_ref, 0)}
    diagonal = []
    for d in range(-REACH, REACH + 1):
        ref, at = tails[d]
        diagonal += [diagonal_rows(ref, at, NB2, i) for i in range(NB2)]
    near = {}
    for d in range(-2, 3):
        ref, at = tails[d]
        near[d] = read_near(ref[at + 2 * NB2 : at + 2 * NB2 + 1, :])

    def weights(j):
        ref, at = matrices[j // NB2 - 2]
        return ref[at + (j % NB2) * ROWS : at + (j % NB2 + 1) * ROWS, :]

    def columns(j):
        return near[j // NB2 - 2][(j % NB2) * K : (j % NB2 + 1) * K]

    def row(d, kind):
        ref, at = tails[d]
        at = at + 2 * NB2 + 1 + kind * NB2
        return jnp.concatenate([ref[at + i : at + i + 1, :] for i in range(NB2)], axis=1).astype(f32).astype(i32)

    return diagonal, weights, columns, row


def third_down_kernel(
    f_ref, p_ref, lo_ref, hi_ref, dlo_ref, dhi_ref, w3_ref, tail_ref, slo_ref, shi_ref, rlo_ref, rhi_ref,
    c_ref, z_ref,
    v0_ref, v1_ref, v2_ref,
):
    diagonal, weights, columns, row = third_fixed(w3_ref, tail_ref, slo_ref, shi_ref, rlo_ref, rhi_ref)
    a, b = NB2, 2 * NB2
    wide = lambda ref, s, i: ref[s + i].astype(f32)
    f = []
    f += [wide(dlo_ref, 0, i) for i in range(a)]
    f += [wide(dlo_ref, a, i) + wide(lo_ref, 0, i) for i in range(a)]
    f += [wide(dlo_ref, b, i) + wide(lo_ref, a, i) + wide(p_ref, 0, i) for i in range(a)]
    f += [f_ref[i] for i in range(a)]
    f += [wide(dhi_ref, b, i) + wide(hi_ref, a, i) + wide(p_ref, b, i) for i in range(a)]
    f += [wide(dhi_ref, a, i) + wide(hi_ref, b, i) for i in range(a)]
    f += [wide(dhi_ref, 0, i) for i in range(a)]
    count = len(f)
    inv = [damping / g for g in diagonal]
    start = [f[i] * inv[i] for i in range(count)]
    for i in range(count):
        v0_ref[i] = start[i].astype(bf16)
    x1 = []
    for j in range(count - 4):
        p = product(v0_ref, [j + c for c in columns(j)], weights(j))
        x1.append(1.2 * start[j + 2] + inv[j + 2] * p)
        v1_ref[j] = x1[j].astype(bf16)
    res = []
    x2 = []
    for j in range(count - 8):
        p = product(v1_ref, [j + c for c in columns(j + 2)], weights(j + 2))
        r = f[j + 4] - diagonal[j + 4] * x1[j + 2] + p
        res.append(r)
        x2.append(x1[j + 2] + inv[j + 4] * r)
        v2_ref[j] = x2[j].astype(bf16)
    left = []
    right = []
    for d in (-1, 0, 1):
        r = jnp.concatenate(res[(d + 1) * a : (d + 2) * a], axis=1)
        left.append(jnp.where(row(d, 0) == -d, r, 0.0).astype(bf16))
        rows = lax.broadcasted_iota(i32, (C3, NB2 * BS), 0)
        right.append(jnp.where(rows == row(d, 1), 1.0, 0.0).astype(bf16))
    c = lax.dot_general(
        jnp.concatenate(left, axis=1), jnp.concatenate(right, axis=1),
        (((1,), (1,)), ((), ())), preferred_element_type=f32,
    ).astype(bf16)
    for i in range(c_ref.shape[0]):
        c_ref[i] = c
    for i in range(a):
        p = product(v2_ref, [i + c for c in columns(i + 4)], weights(i + 4))
        z_ref[i] = 0.2 * x2[i + 2] + start[i + 6] + inv[i + 6] * p


def third_down(copies, *args):
    count = 2 * NB2 * REACH + NB2
    return call(
        third_down_kernel, "down2",
        (shape((copies, R, C3), bf16), shape((NB2, R, BS), f32)),
        [vmem()] * 12, (vmem(),) * 2,
        [
            pltpu.VMEM((count, R, BS), bf16), pltpu.VMEM((count - 4, R, BS), bf16), pltpu.VMEM((count - 8, R, BS), bf16)
        ],
        mib=12, flops=2**27, nbytes=2**21,
    )(*args)


def coarse_kernel(got_ref, z_ref, s_ref, out_ref, copy_ref):
    count = got_ref.shape[0]
    chunks = 4
    size = count // chunks
    u = jnp.zeros((R, C3), f32)
    for c in range(chunks):
        u = u + lax.dot_general(
            joined(got_ref, range(c * size, (c + 1) * size)), s_ref[:, c * size * BS : (c + 1) * size * BS],
            (((1,), (1,)), ((), ())), preferred_element_type=f32,
        )
    out_ref[0] = u.astype(bf16)
    out_ref[1:] = z_ref[...].astype(bf16)
    copy_ref[...] = out_ref[...]


def coarse_solve(got, z, inverse_rows):
    count = got.shape[0]
    return call(
        coarse_kernel, "coarse", (shape((1 + NB2, R, BS), bf16),) * 2,
        [vmem()] * 3, (vmem(),) * 2,
        flops=2**26, nbytes=2**21,
    )(got, z, inverse_rows)


def three_kernel(lo_ref, own_ref, hi_ref, out_ref, copy_ref):
    out_ref[0] = lo_ref[0]
    out_ref[1] = own_ref[0]
    out_ref[2] = hi_ref[0]
    copy_ref[...] = out_ref[...]


def three_of(lo, own, hi):
    return call(
        three_kernel, "three", (shape((3, R, BS), bf16),) * 2, [vmem()] * 3, (vmem(),) * 2,
        flops=2**15, nbytes=2**16,
    )(lo, own, hi)


def third_up_kernel(
    own_ref, lo_ref, hi_ref, ulo_ref, uhi_ref, z_ref, w3_ref, tail_ref, slo_ref, shi_ref, rlo_ref, rhi_ref,
    own2_ref, slot2_ref, x_ref,
    out_ref, first_ref, last_ref,
    v0_ref, v1_ref, e_ref,
):
    diagonal, weights, columns, row = third_fixed(w3_ref, tail_ref, slo_ref, shi_ref, rlo_ref, rhi_ref)
    inv = [damping / g for g in diagonal]
    u = [ulo_ref[0], ulo_ref[1], ulo_ref[2], lo_ref[0], own_ref[0], hi_ref[0], uhi_ref[0], uhi_ref[1], uhi_ref[2]]
    y = []
    for d in range(-REACH, REACH + 1):
        rows = lax.broadcasted_iota(i32, (C3, NB2 * BS), 0)
        pick = jnp.where(rows == row(d, 1), 1.0, 0.0).astype(bf16)
        at = d + REACH
        found = jnp.dot(jnp.concatenate(u[at : at + 3], axis=0), pick, preferred_element_type=f32)
        owner = row(d, 0)
        got = jnp.zeros((R, NB2 * BS), f32)
        for i in range(3):
            got = got + jnp.where(owner == i - 1, found[i * R : (i + 1) * R], 0.0)
        y += [got[:, i * BS : (i + 1) * BS] for i in range(NB2)]
    count = len(y)
    for i in range(count):
        v0_ref[i] = y[i].astype(bf16)
    y1 = []
    for j in range(count - 4):
        p = product(v0_ref, [j + c for c in columns(j)], weights(j))
        y1.append(0.2 * y[j + 2] + inv[j + 2] * p)
        v1_ref[j] = y1[j].astype(bf16)
    for j in range(count - 8):
        p = product(v1_ref, [j + c for c in columns(j + 2)], weights(j + 2))
        y2 = 0.2 * y1[j + 2] + inv[j + 4] * p
        i = j % NB2
        z = (lambda: lo_ref[1 + i].astype(f32), lambda: z_ref[i], lambda: hi_ref[1 + i].astype(f32))[j // NB2]()
        place(e_ref, j, (z + y2).astype(bf16))
    spread(NB1, NB2, e_ref, own2_ref, slot2_ref, device_index(), x_ref, out_ref)
    first_ref[...] = out_ref[:EDGE].astype(bf16)
    last_ref[...] = out_ref[NB1 - EDGE :].astype(bf16)


def third_up(*args):
    count = 2 * NB2 * REACH + NB2
    return call(
        third_up_kernel, "up2",
        (shape((NB1, R, BS), f32), shape((EDGE, R, BS), bf16), shape((EDGE, R, BS), bf16)),
        [vmem()] * 15, (vmem(),) * 3,
        [
            pltpu.VMEM((count, R, BS), bf16), pltpu.VMEM((count - 4, R, BS), bf16),
            pltpu.VMEM((3 * NB2 // 2 * R, 2 * BS), bf16),
        ],
        mib=12, flops=2**27, nbytes=2**21,
    )(*args)


def on_device(
    right_sides,
    weights_fine, columns_fine, degree_fine, owners_fine, slots_fine,
    weights_second, columns_second, degree_second, owners_second, slots_second,
    weights_third, columns_third, degree_third, owners_third, slots_third,
    coarse_inverse,
):
    flat = lambda a: a.reshape(-1, BS)
    f = right_sides
    columns_fine, columns_second, columns_third = columns_fine.T, columns_second.T, columns_third.T
    w1, w2, w3 = (in_hbm(flat(w)) for w in (weights_fine, weights_second, weights_third))
    edges1 = both_ways(*first_edges(in_hbm(flat(f)), w1, in_hbm(degree_fine), in_hbm(columns_fine)))
    g1, g2, _, up, down, w3, tail, kept1, kept2 = fixed_data(
        w1, w2, w3, degree_fine, degree_second, degree_third, columns_second, columns_third, owners_third, slots_third
    )
    fixed = both_ways(up, down)
    far = both_ways(*far_data(w3, tail, *fixed), 2)
    third = (w3, tail, *fixed, *far)

    inner = inner_sweep(NB0, True, columns_fine, f, f, g1, kept1)
    x1, low, mid, high = go_down(
        NB0, NB1, F_ROWS, columns_fine, f, g1, owners_fine, slots_fine, edges1, edges1, kept1, 20, inner
    )
    lo, hi = both_ways(high, low)
    f2, up, down = second_rhs(mid, lo, hi)
    f_edges = both_ways(up, down)
    inner = inner_sweep(NB1, True, columns_second, f2, f2, g2, kept2)
    x2, low, mid, high = go_down(
        NB1, NB2, 0, columns_second, f2, g2, owners_second, slots_second, f_edges, fixed, kept2, 12, inner
    )
    parts, copy = parts_of(low, mid, high)
    plo, phi = both_ways(copy, parts)
    f3, up, down = third_window(mid, parts, plo, phi)
    dlo, dhi = both_ways(up, down, 3)
    c, z = third_down(lax.axis_size("col"), f3, parts, plo, phi, dlo, dhi, *third)
    got = lax.all_to_all(c, "col", 0, 0, tiled=True)
    own, copy = coarse_solve(got, z, coarse_inverse)
    lo, hi = both_ways(copy, own)
    near, copy = three_of(lo, own, hi)
    ulo, uhi = both_ways(near, copy, 3)
    x2, first, last = third_up(own, lo, hi, ulo, uhi, z, *third, owners_second, slots_second, x2)
    x_edges = both_ways(last, first)
    inner = inner_sweep(NB1, False, columns_second, x2, f2, g2, kept2)
    x2, copy = go_up(NB1, 0, columns_second, x2, x_edges, f2, g2, f_edges, fixed, kept2, bf16, 12, 2, inner)
    lo, hi = both_ways(copy, x2)
    x1, first, last = prolong(NB0, NB1, owners_fine, slots_fine, lo, x2, hi, x1)
    x_edges = both_ways(last, first)
    inner = inner_sweep(NB0, False, columns_fine, x1, f, g1, kept1)
    return go_up(NB0, F_ROWS, columns_fine, x1, x_edges, f, g1, edges1, edges1, kept1, f32, 20, 1, inner)[0]


def solution(mesh):
    block = P(AXES, None, None)
    pair = P(AXES, None)
    four = P(AXES, None, None, None)
    level = (four, pair, pair, pair, pair)
    return jax.shard_map(
        on_device, mesh=mesh, in_specs=(block, *level, *level, *level, pair), out_specs=block, check_vma=False
    )
```
